128 devices in a mesh: rows: 32 (over y, x, core), model: 4 (over z).
Axes of the slice: x: 4, y: 4, z: 4, core: 2. Of those that a mesh axis runs over, the one named last changes fastest.
Arguments:
- weight_gate: bfloat16 [2048, 8192], P('rows', 'model'), may hold values from -0.125 to 0.125
- low_gate: bfloat16 [2048, 64], P('rows'), may hold values from -0.125 to 0.125
- high_gate: bfloat16 [64, 8192], P(None, 'model'), may hold values from -0.75 to 0.75
- weight_up: bfloat16 [2048, 8192], P('rows', 'model'), may hold values from -0.125 to 0.125
- low_up: bfloat16 [2048, 64], P('rows'), may hold values from -0.125 to 0.125
- high_up: bfloat16 [64, 8192], P(None, 'model'), may hold values from -0.75 to 0.75
- weight_down: bfloat16 [8192, 2048], P('model', 'rows'), may hold values from -0.0625 to 0.0625
- low_down: bfloat16 [8192, 64], P('model'), may hold values from -0.0625 to 0.0625
- high_down: bfloat16 [64, 2048], P(None, 'rows'), may hold values from -0.75 to 0.75
- norm_train: float32 [2048], P(('rows', 'model')), may hold values from 0.25 to 1.75
- norm_step: float32 [2048], P(('rows', 'model')), may hold values from -0.3 to 0.3
Outputs:
- final_gate: bfloat16 [8192, 2048], P('model')
- final_up: bfloat16 [8192, 2048], P('model')
- final_down: bfloat16 [2048, 8192], P(None, 'model')
- serve_norm: bfloat16 [2048], replicated
The draws below stay inside these ranges and needn't reach their ends.
All inputs are finite; a program needn't handle non-finite values.
Results may differ from the reference program's by a relative error of at most 0.001.
Values may be sent and summed in bfloat16 or wider, within the bound.
A program may use at most 192 MiB of HBM per device.

```python
import jax
import jax.numpy as jnp

D_MODEL = 2048
D_INNER = 8192
RANK = 64


def block_scale(own_key, extent, split, least, top_value):
    def one(position, shards_of):
        steps = jax.random.uniform(jax.random.fold_in(jax.random.fold_in(own_key, 6), position), (shards_of,), jnp.float32, least / len(split), top_value / len(split))
        return jnp.repeat(jnp.exp(steps), extent[position] // shards_of).reshape((-1,) + (1,) * (len(extent) - position - 1))

    level = one(*split[0])
    for cut in split[1:]:
        level = level * one(*cut)
    return level


def bell_draw(rng, shape, scale, limit, pieces=(), dtype=jnp.bfloat16):
    drawn = jax.random.normal(rng, shape, jnp.float32) * scale
    if len(pieces) > 0:
        drawn = block_scale(rng, shape, pieces, -0.22, 0.18) * drawn
    return jnp.clip(drawn, min=-limit, max=limit).astype(dtype)


def setup_inputs(seed: int = 0) -> dict:
    keys = jax.random.split(jax.random.key(seed), 12)
    return {
        "weight_gate": bell_draw(keys[0], (D_MODEL, D_INNER), D_MODEL ** -0.5, 0.125, ((0, 32), (1, 4))),
        "low_gate": bell_draw(keys[1], (D_MODEL, RANK), D_MODEL ** -0.5, 0.125, ((0, 32),)),
        "high_gate": bell_draw(keys[2], (RANK, D_INNER), RANK ** -0.5, 0.75, ((1, 4),)),
        "weight_up": bell_draw(keys[3], (D_MODEL, D_INNER), D_MODEL ** -0.5, 0.125, ((0, 32), (1, 4))),
        "low_up": bell_draw(keys[4], (D_MODEL, RANK), D_MODEL ** -0.5, 0.125, ((0, 32),)),
        "high_up": bell_draw(keys[5], (RANK, D_INNER), RANK ** -0.5, 0.75, ((1, 4),)),
        "weight_down": bell_draw(keys[6], (D_INNER, D_MODEL), D_INNER ** -0.5, 0.0625, ((0, 4), (1, 32))),
        "low_down": bell_draw(keys[7], (D_INNER, RANK), D_INNER ** -0.5, 0.0625, ((0, 4),)),
        "high_down": bell_draw(keys[8], (RANK, D_MODEL), RANK ** -0.5, 0.75, ((1, 32),)),
        "norm_train": jnp.clip(1.0 + 0.15 * jax.random.normal(keys[9], (D_MODEL,), jnp.float32), 0.25, 1.75),
        "norm_step": jnp.clip(jax.random.uniform(keys[10], (D_MODEL,), jnp.float32, -0.3, 0.3) * block_scale(keys[10], (D_MODEL,), ((0, 128),), -0.4, 0.0), -0.3, 0.3),
    }


mix_rate = 0.5


def reference(weight_gate, low_gate, high_gate, weight_up, low_up, high_up, weight_down, low_down, high_down, norm_train, norm_step):
    result_gate = weight_gate.astype(jnp.float32) + mix_rate * jnp.dot(low_gate, high_gate, preferred_element_type=jnp.float32)
    result_up = weight_up.astype(jnp.float32) + mix_rate * jnp.dot(low_up, high_up, preferred_element_type=jnp.float32)
    result_down = weight_down.astype(jnp.float32) + mix_rate * jnp.dot(low_down, high_down, preferred_element_type=jnp.float32)
    final_gate = result_gate.T.astype(jnp.bfloat16)
    final_up = result_up.T.astype(jnp.bfloat16)
    final_down = result_down.T.astype(jnp.bfloat16)
    serve_norm = (norm_train + norm_step).astype(jnp.bfloat16)
    return final_gate, final_up, final_down, serve_norm
```

```python
import functools

import jax
import jax.numpy as jnp
from jax import lax
from jax.experimental import pallas as pl
from jax.experimental.pallas import tpu as pltpu
from jax.sharding import Mesh
from jax.sharding import PartitionSpec as P

ROWS = ("rows_0", "rows_1", "rows_2")
ROWS_MODEL = ("rows_0", "rows_1", "rows_2", "model")
MESH = pl.DeviceIdType.MESH

mix_rate = 0.5

TREES = (("x", 1), ("x", -1), ("y", 1), ("y", -1))
DOWN, GATE, UP = 0, 1, 2


def tree_slots(sign):
    steps = (0, sign, -sign, 2 * sign)
    hops = {0: 0, sign: 1, -sign: 1, 2 * sign: 2}
    slots = [(a, b) for a in steps for b in steps if (a, b) != (0, 0)]
    return sorted(slots, key=lambda s: (hops[s[0]] + hops[s[1]], hops[s[1]]))


def onward(a, b, sign):
    places = []
    if b == 0:
        if a == 0:
            places += [(sign, 0), (-sign, 0)]
        elif a == sign:
            places += [(2 * sign, 0)]
        places += [(a, sign), (a, -sign)]
    elif b == sign:
        places += [(a, 2 * sign)]
    return places


def slot_number(a, b):
    return (a % 4) * 4 + b % 4


def gather_kernel(
    wd_in, ld_in, hd_in, wg_in, lg_in, hg_in, wu_in, lu_in, hu_in, train_in, step_in,
    down, gate, up, norm,
    wd, ld, hd, wg, lg, hg, wu, lu, hu, train, step, row, part, zrow,
    in_sem, part_send, part_recv, send_sem, side_send, side_recv, recv_sem,
    n_send, n_recv,
):
    y, x, k, z = (lax.axis_index(n) for n in ROWS_MODEL)
    other = 1 - k
    chip = y * 4 + x

    def toward(axis, by):
        if axis == "x":
            return {"rows_1": lax.rem(x + by + 4, 4)}
        if axis == "y":
            return {"rows_0": lax.rem(y + by + 4, 4)}
        return {"model": lax.rem(z + by + 4, 4)}

    partner = {"rows_2": other}

    half = pl.ds(pl.multiple_of(k * 1024, 1024), 1024)
    half_other = pl.ds(pl.multiple_of(other * 1024, 1024), 1024)
    mine = pl.ds(pl.multiple_of(k * 64, 64), 64)
    reads = [
        pltpu.make_async_copy(s, d, in_sem.at[i])
        for i, (s, d) in enumerate(
            [
                (wd_in, wd), (ld_in, ld), (hd_in, hd),
                (wg_in.at[:, half], wg.at[mine]), (lg_in, lg.at[mine]), (hg_in.at[:, half], hg),
                (wu_in.at[:, half], wu.at[mine]), (lu_in, lu.at[mine]), (hu_in.at[:, half], hu),
                (train_in, train), (step_in, step),
            ]
        )
    ]
    for r in reads:
        r.start()

    barrier = pltpu.get_barrier_semaphore()
    peers = [partner] + [toward(axis, by) for axis in "xyz" for by in (1, -1)]
    for p in peers:
        pl.semaphore_signal(barrier, inc=1, device_id=p, device_id_type=MESH)

    lane = lax.broadcasted_iota(jnp.int32, (1, 128), 1)
    first = k * 64 + z * 16
    reads[9].wait()
    reads[10].wait()
    own = jnp.zeros((1, 128), jnp.float32)
    for i in range(16):
        own = jnp.where(lane == first + i, train[i] + step[i], own)
    row[...] = own

    pl.semaphore_wait(barrier, len(peers))

    def to_partner(i, src, dst):
        return pltpu.make_async_remote_copy(
            src_ref=src, dst_ref=dst, send_sem=part_send.at[i], recv_sem=part_recv.at[i],
            device_id=partner, device_id_type=MESH,
        )

    swaps = [
        to_partner(0, wg_in.at[:, half_other], wg.at[mine]),
        to_partner(1, lg_in, lg.at[mine]),
        to_partner(2, wu_in.at[:, half_other], wu.at[mine]),
        to_partner(3, lu_in, lu.at[mine]),
        to_partner(4, row, part),
    ]
    for s in swaps:
        s.start()

    def piece(arr, t, c):
        if arr == DOWN:
            return down.at[c, k, pl.ds(16 * t, 16), :]
        ref = gate if arr == GATE else up
        return ref.at[k, t, :, pl.ds(pl.multiple_of(c * 128, 128), 128)]

    def origin(t, a, b):
        dx, dy = (a, b) if TREES[t][0] == "x" else (b, a)
        return lax.rem(y - dy + 4, 4) * 4 + lax.rem(x - dx + 4, 4)

    def copy_on(arr, t, a, b, c, na, nb):
        first_axis = TREES[t][0]
        second_axis = "y" if first_axis == "x" else "x"
        sign = TREES[t][1]
        if na != a:
            axis, by = first_axis, (-sign if na == -sign else sign)
        else:
            axis, by = second_axis, (-sign if nb == -sign else sign)
        ref = piece(arr, t, c)
        return pltpu.make_async_remote_copy(
            src_ref=ref, dst_ref=ref, send_sem=send_sem.at[arr],
            recv_sem=recv_sem.at[(arr * 4 + t) * 16 + slot_number(na, nb)],
            device_id=toward(axis, by), device_id_type=MESH,
        )

    def send_on(arr, t, a, b, c):
        for na, nb in onward(a, b, TREES[t][1]):
            copy_on(arr, t, a, b, c, na, nb).start()
        ref = piece(arr, t, c)
        pltpu.make_async_remote_copy(
            src_ref=ref, dst_ref=ref, send_sem=side_send.at[arr], recv_sem=side_recv.at[arr],
            device_id=partner, device_id_type=MESH,
        ).start()

    def arrive(arr, t, a, b):
        c = origin(t, a, b)
        ref = piece(arr, t, c)
        pltpu.make_async_remote_copy(
            src_ref=ref, dst_ref=ref, send_sem=send_sem.at[arr],
            recv_sem=recv_sem.at[(arr * 4 + t) * 16 + slot_number(a, b)],
            device_id=partner, device_id_type=MESH,
        ).wait_recv()
        send_on(arr, t, a, b, c)

    for i in range(3):
        reads[i].wait()
    mix = lax.dot_general(hd[...], ld[...], (((0,), (0,)), ((), ())), preferred_element_type=jnp.float32)
    down[chip, k] = (wd[...].astype(jnp.float32) + mix_rate * mix).astype(jnp.bfloat16)
    swaps[4].wait()
    zrow[0] = row[...] + part[...]
    for t in range(4):
        send_on(DOWN, t, 0, 0, chip)

    def turned(ref, w, low, high):
        for t in range(4):
            cols = pl.ds(256 * t, 256)
            mix = jnp.dot(low[...], high[:, cols], preferred_element_type=jnp.float32)
            full = w[:, cols].astype(jnp.float32) + mix_rate * mix
            ref[k, t, :, pl.ds(pl.multiple_of(chip * 128, 128), 128)] = full.T.astype(jnp.bfloat16)

    for i in (3, 4, 5):
        reads[i].wait()
    swaps[0].wait()
    swaps[1].wait()
    turned(gate, wg, lg, hg)

    def norm_copy(src, dst, slot, to):
        return pltpu.make_async_remote_copy(
            src_ref=src, dst_ref=dst, send_sem=n_send.at[slot], recv_sem=n_recv.at[slot],
            device_id=to, device_id_type=MESH,
        )

    z_up = norm_copy(zrow.at[0], zrow.at[1], 16, toward("z", 1))
    z_down = norm_copy(zrow.at[0], zrow.at[2], 17, toward("z", -1))
    z_far = norm_copy(zrow.at[1], zrow.at[3], 18, toward("z", 1))
    z_up.start()
    z_down.start()

    for t in range(4):
        send_on(GATE, t, 0, 0, chip)

    for i in (6, 7, 8):
        reads[i].wait()
    swaps[2].wait()
    swaps[3].wait()
    turned(up, wu, lu, hu)
    z_up.wait()
    z_far.start()

    def each(arr):
        order = tree_slots(1)
        return [(arr, t, TREES[t][1] * a, TREES[t][1] * b) for a, b in order for t in range(4)]

    for e in each(DOWN):
        arrive(*e)

    z_down.wait()
    z_far.wait()
    norm[chip] = zrow[0] + zrow[1] + zrow[2] + zrow[3]

    for t in range(4):
        send_on(UP, t, 0, 0, chip)

    def norm_on(a, b, c):
        sign = TREES[0][1]
        for na, nb in onward(a, b, sign):
            if na != a:
                to = toward("x", -sign if na == -sign else sign)
            else:
                to = toward("y", -sign if nb == -sign else sign)
            norm_copy(norm.at[c], norm.at[c], slot_number(na, nb), to).start()

    def norm_arrive(a, b):
        c = origin(0, a, b)
        norm_copy(norm.at[c], norm.at[c], slot_number(a, b), partner).wait_recv()
        norm_on(a, b, c)

    norm_on(0, 0, chip)
    for e in each(GATE):
        arrive(*e)
    for a, b in tree_slots(TREES[0][1]):
        norm_arrive(a, b)
    for e in each(UP):
        arrive(*e)

    for a, b in tree_slots(TREES[0][1]):
        norm_copy(norm.at[0], norm.at[0], slot_number(a, b), partner).wait_send()

    def drain(arr, ref, part_send_ref, other_half, own_half):
        pltpu.make_async_copy(part_send_ref, part_send_ref, send_sem.at[arr]).wait()
        pltpu.make_async_copy(own_half, own_half, side_send.at[arr]).wait()
        pltpu.make_async_copy(other_half, other_half, side_recv.at[arr]).wait()

    drain(DOWN, down, down.at[pl.ds(0, 15), k], down.at[:, other], down.at[:, k])
    drain(GATE, gate, gate.at[k, :, :, pl.ds(0, 1920)], gate.at[other], gate.at[k])
    drain(UP, up, up.at[k, :, :, pl.ds(0, 1920)], up.at[other], up.at[k])


def write_kernel(down, gate, up, norm, down_out, gate_out, up_out, norm_out, sem):
    copies = []
    for n, (src, dst) in enumerate([(gate, gate_out), (up, up_out)]):
        for h in range(2):
            for t in range(4):
                copies.append((src.at[h, t], dst.at[h, t]))
    for q in range(8):
        rows = pl.ds(2 * q, 2)
        copies.append((down.at[rows], down_out.at[rows]))
    copies = [pltpu.make_async_copy(s, d, sem.at[i]) for i, (s, d) in enumerate(copies)]
    for c in copies:
        c.start()
    norm_out[...] = norm[...].reshape(16, 128).astype(jnp.bfloat16)
    for c in copies:
        c.wait()


def local(
    weight_gate, low_gate, high_gate, weight_up, low_up, high_up,
    weight_down, low_down, high_down, norm_train, norm_step,
):
    bf16, f32 = jnp.bfloat16, jnp.float32
    hbm = pl.BlockSpec(memory_space=pltpu.HBM)
    vmem = pl.BlockSpec(memory_space=pltpu.VMEM)
    dma = pltpu.SemaphoreType.DMA
    down, gate, up, norm = pl.pallas_call(
        gather_kernel,
        out_shape=(
            pltpu.VMEM((16, 2, 64, 2048), bf16),
            pltpu.VMEM((2, 4, 256, 2048), bf16),
            pltpu.VMEM((2, 4, 256, 2048), bf16),
            pltpu.VMEM((16, 1, 128), f32),
        ),
        in_specs=[hbm] * 11,
        out_specs=(vmem,) * 4,
        scratch_shapes=[
            pltpu.VMEM((64, 2048), bf16), pltpu.VMEM((64, 2048), bf16), pltpu.VMEM((64, 64), bf16),
            pltpu.VMEM((128, 1024), bf16), pltpu.VMEM((128, 64), bf16), pltpu.VMEM((64, 1024), bf16),
            pltpu.VMEM((128, 1024), bf16), pltpu.VMEM((128, 64), bf16), pltpu.VMEM((64, 1024), bf16),
            pltpu.SMEM((16,), f32), pltpu.SMEM((16,), f32),
            pltpu.VMEM((1, 128), f32), pltpu.VMEM((1, 128), f32), pltpu.VMEM((4, 1, 128), f32),
            dma((11,)), dma((5,)), dma((5,)), dma((3,)), dma((3,)), dma((3,)), dma((192,)),
            dma((19,)), dma((19,)),
        ],
        compiler_params=pltpu.CompilerParams(
            collective_id=0, has_side_effects=True, vmem_limit_bytes=8 << 20
        ),
        name="gather",
    )(*(
        pltpu.with_memory_space_constraint(a, pltpu.HBM)
        for a in (
            weight_down.T, low_down.T, high_down, weight_gate, low_gate, high_gate,
            weight_up, low_up, high_up, norm_train, norm_step,
        )
    ))
    down, gate, up, norm = pl.pallas_call(
        write_kernel,
        out_shape=(
            jax.ShapeDtypeStruct((16, 2, 64, 2048), bf16),
            jax.ShapeDtypeStruct((2, 4, 256, 2048), bf16),
            jax.ShapeDtypeStruct((2, 4, 256, 2048), bf16),
            jax.ShapeDtypeStruct((16, 128), bf16),
        ),
        in_specs=[vmem] * 4,
        out_specs=(hbm, hbm, hbm, vmem),
        scratch_shapes=[dma((24,))],
        compiler_params=pltpu.CompilerParams(vmem_limit_bytes=4 << 20),
        name="write",
    )(down, gate, up, norm)
    return gate.reshape(2048, 2048), up.reshape(2048, 2048), down.reshape(2048, 2048), norm.reshape(2048)


def solution(mesh):
    split = Mesh(
        mesh.devices.reshape(4, 4, 2, mesh.shape["model"]), ROWS_MODEL
    )
    placed = (
        P(ROWS, "model"),
        P(ROWS, None),
        P(None, "model"),
        P(ROWS, "model"),
        P(ROWS, None),
        P(None, "model"),
        P("model", ROWS),
        P("model", None),
        P(None, ROWS),
        P(ROWS_MODEL),
        P(ROWS_MODEL),
    )
    return jax.shard_map(
        local,
        mesh=split,
        in_specs=placed,
        out_specs=(P("model", None), P("model", None), P(None, "model"), P()),
        check_vma=False,
    )
```

```python
import functools

import jax
import jax.numpy as jnp
from jax import lax
from jax.experimental import pallas as pl
from jax.experimental.pallas import tpu as pltpu
from jax.sharding import Mesh
from jax.sharding import PartitionSpec as P

ROWS = ("rows_0", "rows_1", "rows_2")
ROWS_MODEL = ("rows_0", "rows_1", "rows_2", "model")
MESH = pl.DeviceIdType.MESH

mix_rate = 0.5

TREES = (("x", 1), ("x", -1), ("y", 1), ("y", -1))
DOWN, GATE, UP = 0, 1, 2


def tree_slots(sign):
    steps = (0, sign, -sign, 2 * sign)
    hops = {0: 0, sign: 1, -sign: 1, 2 * sign: 2}
    slots = [(a, b) for a in steps for b in steps if (a, b) != (0, 0)]
    return sorted(slots, key=lambda s: (hops[s[0]] + hops[s[1]], hops[s[1]]))


def onward(a, b, sign):
    places = []
    if b == 0:
        if a == 0:
            places += [(sign, 0), (-sign, 0)]
        elif a == sign:
            places += [(2 * sign, 0)]
        places += [(a, sign), (a, -sign)]
    elif b == sign:
        places += [(a, 2 * sign)]
    return places


def slot_number(a, b):
    return (a % 4) * 4 + b % 4


def gather_kernel(
    wd_in, ld_in, hd_in, wg_in, lg_in, hg_in, wu_in, lu_in, hu_in, train_in, step_in,
    down, gate, up, norm,
    wd, ld, hd, wg, lg, hg, wu, lu, hu, train, step, row, part, zrow,
    in_sem, part_send, part_recv, send_sem, side_send, side_recv, recv_sem,
    n_send, n_recv,
):
    y, x, k, z = (lax.axis_index(n) for n in ROWS_MODEL)
    other = 1 - k
    chip = y * 4 + x

    def toward(axis, by):
        if axis == "x":
            return {"rows_1": lax.rem(x + by + 4, 4)}
        if axis == "y":
            return {"rows_0": lax.rem(y + by + 4, 4)}
        return {"model": lax.rem(z + by + 4, 4)}

    partner = {"rows_2": other}

    half = pl.ds(pl.multiple_of(k * 1024, 1024), 1024)
    half_other = pl.ds(pl.multiple_of(other * 1024, 1024), 1024)
    mine = pl.ds(pl.multiple_of(k * 64, 64), 64)
    reads = [
        pltpu.make_async_copy(s, d, in_sem.at[i])
        for i, (s, d) in enumerate(
            [
                (wd_in, wd), (ld_in, ld), (hd_in, hd),
                (wg_in.at[:, half], wg.at[mine]), (lg_in, lg.at[mine]), (hg_in.at[:, half], hg),
                (wu_in.at[:, half], wu.at[mine]), (lu_in, lu.at[mine]), (hu_in.at[:, half], hu),
                (train_in, train), (step_in, step),
            ]
        )
    ]
    for r in reads:
        r.start()

    barrier = pltpu.get_barrier_semaphore()
    peers = [partner] + [toward(axis, by) for axis in "xyz" for by in (1, -1)]
    for p in peers:
        pl.semaphore_signal(barrier, inc=1, device_id=p, device_id_type=MESH)

    lane = lax.broadcasted_iota(jnp.int32, (1, 128), 1)
    first = k * 64 + z * 16
    reads[9].wait()
    reads[10].wait()
    own = jnp.zeros((1, 128), jnp.float32)
    for i in range(16):
        own = jnp.where(lane == first + i, train[i] + step[i], own)
    row[...] = own

    pl.semaphore_wait(barrier, len(peers))

    def to_partner(i, src, dst):
        return pltpu.make_async_remote_copy(
            src_ref=src, dst_ref=dst, send_sem=part_send.at[i], recv_sem=part_recv.at[i],
            device_id=partner, device_id_type=MESH,
        )

    swaps = [
        to_partner(0, wg_in.at[:, half_other], wg.at[mine]),
        to_partner(1, lg_in, lg.at[mine]),
        to_partner(2, wu_in.at[:, half_other], wu.at[mine]),
        to_partner(3, lu_in, lu.at[mine]),
        to_partner(4, row, part),
    ]
    for s in swaps:
        s.start()

    def piece(arr, t, c):
        if arr == DOWN:
            return down.at[c, k, pl.ds(16 * t, 16), :]
        ref = gate if arr == GATE else up
        return ref.at[k, t, :, pl.ds(pl.multiple_of(c * 128, 128), 128)]

    def origin(t, a, b):
        dx, dy = (a, b) if TREES[t][0] == "x" else (b, a)
        return lax.rem(y - dy + 4, 4) * 4 + lax.rem(x - dx + 4, 4)

    def copy_on(arr, t, a, b, c, na, nb):
        first_axis = TREES[t][0]
        second_axis = "y" if first_axis == "x" else "x"
        sign = TREES[t][1]
        if na != a:
            axis, by = first_axis, (-sign if na == -sign else sign)
        else:
            axis, by = second_axis, (-sign if nb == -sign else sign)
        ref = piece(arr, t, c)
        return pltpu.make_async_remote_copy(
            src_ref=ref, dst_ref=ref, send_sem=send_sem.at[arr],
            recv_sem=recv_sem.at[(arr * 4 + t) * 16 + slot_number(na, nb)],
            device_id=toward(axis, by), device_id_type=MESH,
        )

    def send_on(arr, t, a, b, c):
        for na, nb in onward(a, b, TREES[t][1]):
            copy_on(arr, t, a, b, c, na, nb).start()
        ref = piece(arr, t, c)
        pltpu.make_async_remote_copy(
            src_ref=ref, dst_ref=ref, send_sem=side_send.at[arr], recv_sem=side_recv.at[arr],
            device_id=partner, device_id_type=MESH,
        ).start()

    def arrive(arr, t, a, b):
        c = origin(t, a, b)
        ref = piece(arr, t, c)
        pltpu.make_async_remote_copy(
            src_ref=ref, dst_ref=ref, send_sem=send_sem.at[arr],
            recv_sem=recv_sem.at[(arr * 4 + t) * 16 + slot_number(a, b)],
            device_id=partner, device_id_type=MESH,
        ).wait_recv()
        send_on(arr, t, a, b, c)

    for i in range(3):
        reads[i].wait()
    mix = lax.dot_general(hd[...], ld[...], (((0,), (0,)), ((), ())), preferred_element_type=jnp.float32)
    down[chip, k] = (wd[...].astype(jnp.float32) + mix_rate * mix).astype(jnp.bfloat16)
    swaps[4].wait()
    zrow[0] = row[...] + part[...]
    for t in range(4):
        send_on(DOWN, t, 0, 0, chip)

    def turned(ref, w, low, high):
        for t in range(4):
            cols = pl.ds(256 * t, 256)
            mix = jnp.dot(low[...], high[:, cols], preferred_element_type=jnp.float32)
            full = w[:, cols].astype(jnp.float32) + mix_rate * mix
            ref[k, t, :, pl.ds(pl.multiple_of(chip * 128, 128), 128)] = full.T.astype(jnp.bfloat16)

    for i in (3, 4, 5):
        reads[i].wait()
    swaps[0].wait()
    swaps[1].wait()
    turned(gate, wg, lg, hg)

    def norm_copy(src, dst, slot, to):
        return pltpu.make_async_remote_copy(
            src_ref=src, dst_ref=dst, send_sem=n_send.at[slot], recv_sem=n_recv.at[slot],
            device_id=to, device_id_type=MESH,
        )

    z_up = norm_copy(zrow.at[0], zrow.at[1], 16, toward("z", 1))
    z_down = norm_copy(zrow.at[0], zrow.at[2], 17, toward("z", -1))
    z_far = norm_copy(zrow.at[1], zrow.at[3], 18, toward("z", 1))
    z_up.start()
    z_down.start()

    for t in range(4):
        send_on(GATE, t, 0, 0, chip)

    for i in (6, 7, 8):
        reads[i].wait()
    swaps[2].wait()
    swaps[3].wait()
    turned(up, wu, lu, hu)
    for t in range(4):
        send_on(UP, t, 0, 0, chip)
    z_up.wait()
    z_far.start()

    def level(hops):
        signs = [(a, b) for a, b in tree_slots(1) if abs(a) + abs(b) == hops]
        return [
            (arr, t, TREES[t][1] * a, TREES[t][1] * b)
            for arr in (DOWN, GATE, UP) for a, b in signs for t in range(4)
        ]

    def norm_on(a, b, c):
        sign = TREES[0][1]
        for na, nb in onward(a, b, sign):
            if na != a:
                to = toward("x", -sign if na == -sign else sign)
            else:
                to = toward("y", -sign if nb == -sign else sign)
            norm_copy(norm.at[c], norm.at[c], slot_number(na, nb), to).start()

    def norm_arrive(a, b):
        c = origin(0, a, b)
        norm_copy(norm.at[c], norm.at[c], slot_number(a, b), partner).wait_recv()
        norm_on(a, b, c)

    for e in level(1):
        arrive(*e)
    z_down.wait()
    z_far.wait()
    norm[chip] = zrow[0] + zrow[1] + zrow[2] + zrow[3]
    norm_on(0, 0, chip)
    for hops in (2, 3, 4):
        for e in level(hops):
            arrive(*e)
        for a, b in tree_slots(TREES[0][1]):
            if abs(a) + abs(b) == hops - 1:
                norm_arrive(a, b)
    norm_arrive(2, 2)

    for a, b in tree_slots(TREES[0][1]):
        norm_copy(norm.at[0], norm.at[0], slot_number(a, b), partner).wait_send()

    def drain(arr, ref, part_send_ref, other_half, own_half):
        pltpu.make_async_copy(part_send_ref, part_send_ref, send_sem.at[arr]).wait()
        pltpu.make_async_copy(own_half, own_half, side_send.at[arr]).wait()
        pltpu.make_async_copy(other_half, other_half, side_recv.at[arr]).wait()

    drain(DOWN, down, down.at[pl.ds(0, 15), k], down.at[:, other], down.at[:, k])
    drain(GATE, gate, gate.at[k, :, :, pl.ds(0, 1920)], gate.at[other], gate.at[k])
    drain(UP, up, up.at[k, :, :, pl.ds(0, 1920)], up.at[other], up.at[k])


def write_kernel(down, gate, up, norm, down_out, gate_out, up_out, norm_out, sem):
    copies = []
    for n, (src, dst) in enumerate([(gate, gate_out), (up, up_out)]):
        for h in range(2):
            for t in range(4):
                copies.append((src.at[h, t], dst.at[h, t]))
    for q in range(8):
        rows = pl.ds(2 * q, 2)
        copies.append((down.at[rows], down_out.at[rows]))
    copies = [pltpu.make_async_copy(s, d, sem.at[i]) for i, (s, d) in enumerate(copies)]
    for c in copies:
        c.start()
    norm_out[...] = norm[...].reshape(16, 128).astype(jnp.bfloat16)
    for c in copies:
        c.wait()


def local(
    weight_gate, low_gate, high_gate, weight_up, low_up, high_up,
    weight_down, low_down, high_down, norm_train, norm_step,
):
    bf16, f32 = jnp.bfloat16, jnp.float32
    hbm = pl.BlockSpec(memory_space=pltpu.HBM)
    vmem = pl.BlockSpec(memory_space=pltpu.VMEM)
    dma = pltpu.SemaphoreType.DMA
    down, gate, up, norm = pl.pallas_call(
        gather_kernel,
        out_shape=(
            pltpu.VMEM((16, 2, 64, 2048), bf16),
            pltpu.VMEM((2, 4, 256, 2048), bf16),
            pltpu.VMEM((2, 4, 256, 2048), bf16),
            pltpu.VMEM((16, 1, 128), f32),
        ),
        in_specs=[hbm] * 11,
        out_specs=(vmem,) * 4,
        scratch_shapes=[
            pltpu.VMEM((64, 2048), bf16), pltpu.VMEM((64, 2048), bf16), pltpu.VMEM((64, 64), bf16),
            pltpu.VMEM((128, 1024), bf16), pltpu.VMEM((128, 64), bf16), pltpu.VMEM((64, 1024), bf16),
            pltpu.VMEM((128, 1024), bf16), pltpu.VMEM((128, 64), bf16), pltpu.VMEM((64, 1024), bf16),
            pltpu.SMEM((16,), f32), pltpu.SMEM((16,), f32),
            pltpu.VMEM((1, 128), f32), pltpu.VMEM((1, 128), f32), pltpu.VMEM((4, 1, 128), f32),
            dma((11,)), dma((5,)), dma((5,)), dma((3,)), dma((3,)), dma((3,)), dma((192,)),
            dma((19,)), dma((19,)),
        ],
        compiler_params=pltpu.CompilerParams(
            collective_id=0, has_side_effects=True, vmem_limit_bytes=8 << 20
        ),
        name="gather",
    )(*(
        pltpu.with_memory_space_constraint(a, pltpu.HBM)
        for a in (
            weight_down.T, low_down.T, high_down, weight_gate, low_gate, high_gate,
            weight_up, low_up, high_up, norm_train, norm_step,
        )
    ))
    down, gate, up, norm = pl.pallas_call(
        write_kernel,
        out_shape=(
            jax.ShapeDtypeStruct((16, 2, 64, 2048), bf16),
            jax.ShapeDtypeStruct((2, 4, 256, 2048), bf16),
            jax.ShapeDtypeStruct((2, 4, 256, 2048), bf16),
            jax.ShapeDtypeStruct((16, 128), bf16),
        ),
        in_specs=[vmem] * 4,
        out_specs=(hbm, hbm, hbm, vmem),
        scratch_shapes=[dma((24,))],
        compiler_params=pltpu.CompilerParams(vmem_limit_bytes=4 << 20),
        name="write",
    )(down, gate, up, norm)
    return gate.reshape(2048, 2048), up.reshape(2048, 2048), down.reshape(2048, 2048), norm.reshape(2048)


def solution(mesh):
    split = Mesh(
        mesh.devices.reshape(4, 4, 2, mesh.shape["model"]), ROWS_MODEL
    )
    placed = (
        P(ROWS, "model"),
        P(ROWS, None),
        P(None, "model"),
        P(ROWS, "model"),
        P(ROWS, None),
        P(None, "model"),
        P("model", ROWS),
        P("model", None),
        P(None, ROWS),
        P(ROWS_MODEL),
        P(ROWS_MODEL),
    )
    return jax.shard_map(
        local,
        mesh=split,
        in_specs=placed,
        out_specs=(P("model", None), P("model", None), P(None, "model"), P()),
        check_vma=False,
    )
```

```python
import functools

import jax
import jax.numpy as jnp
from jax import lax
from jax.experimental import pallas as pl
from jax.experimental.pallas import tpu as pltpu
from jax.sharding import Mesh
from jax.sharding import PartitionSpec as P

ROWS = ("rows_0", "rows_1", "rows_2")
ROWS_MODEL = ("rows_0", "rows_1", "rows_2", "model")
MESH = pl.DeviceIdType.MESH

mix_rate = 0.5

TREES = (("x", 1), ("x", -1), ("y", 1), ("y", -1))
DOWN, GATE, UP = 0, 1, 2


def tree_slots(sign):
    steps = (0, sign, -sign, 2 * sign)
    hops = {0: 0, sign: 1, -sign: 1, 2 * sign: 2}
    slots = [(a, b) for a in steps for b in steps if (a, b) != (0, 0)]
    return sorted(slots, key=lambda s: (hops[s[0]] + hops[s[1]], hops[s[1]]))


def onward(a, b, sign):
    places = []
    if b == 0:
        if a == 0:
            places += [(sign, 0), (-sign, 0)]
        elif a == sign:
            places += [(2 * sign, 0)]
        places += [(a, sign), (a, -sign)]
    elif b == sign:
        places += [(a, 2 * sign)]
    return places


def slot_number(a, b):
    return (a % 4) * 4 + b % 4


WAYS = (("x", 1), ("x", -1), ("y", 1), ("y", -1), ("x", 2), ("y", 2))
BACK = (1, 0, 3, 2, 4, 5)


def gather_kernel(
    wd_in, ld_in, hd_in, wg_in, lg_in, hg_in, wu_in, lu_in, hu_in, train_in, step_in,
    down, gate, up, norm_out,
    wd, ld, hd, wg, lg, hg, wu, lu, hu, train, step, norm, part, total, below, above, tosend,
    in_sem, part_send, part_recv, send_sem, side_send, side_recv, recv_sem,
    n_send, n_recv, ready,
):
    y, x, k, z = (lax.axis_index(n) for n in ROWS_MODEL)
    other = 1 - k
    chip = y * 4 + x
    place = {"x": x, "y": y}

    def toward(axis, by):
        if axis == "x":
            return {"rows_1": lax.rem(x + by + 4, 4)}
        if axis == "y":
            return {"rows_0": lax.rem(y + by + 4, 4)}
        return {"model": lax.rem(z + by + 4, 4)}

    partner = {"rows_2": other}

    half = pl.ds(pl.multiple_of(k * 1024, 1024), 1024)
    half_other = pl.ds(pl.multiple_of(other * 1024, 1024), 1024)
    mine = pl.ds(pl.multiple_of(k * 64, 64), 64)
    reads = [
        pltpu.make_async_copy(s, d, in_sem.at[i])
        for i, (s, d) in enumerate(
            [
                (wd_in, wd), (ld_in, ld), (hd_in, hd),
                (wg_in.at[:, half], wg.at[mine]), (lg_in, lg.at[mine]), (hg_in.at[:, half], hg),
                (wu_in.at[:, half], wu.at[mine]), (lu_in, lu.at[mine]), (hu_in.at[:, half], hu),
                (train_in, train), (step_in, step),
            ]
        )
    ]
    for r in reads:
        r.start()
    below[...] = jnp.zeros_like(below)
    above[...] = jnp.zeros_like(above)

    def later(way):
        axis, by = WAYS[way]
        p = place[axis]
        return (p == 0) | (p == 3) if by == -1 else p < 2

    barrier = pltpu.get_barrier_semaphore()
    pl.semaphore_signal(barrier, inc=1, device_id=partner, device_id_type=MESH)
    for w in range(6):
        @pl.when(later(w))
        def _(w=w):
            pl.semaphore_signal(barrier, inc=1, device_id=toward(*WAYS[w]), device_id_type=MESH)

    @pl.when(z < 3)
    def _():
        pl.semaphore_signal(barrier, inc=1, device_id=toward("z", 1), device_id_type=MESH)

    one, nil = jnp.int32(1), jnp.int32(0)
    greetings = 1 + jnp.where(z > 0, one, nil)
    for w in range(6):
        greetings = greetings + jnp.where(later(w), nil, one)
    pl.semaphore_wait(barrier, greetings)
    for w in range(6):
        @pl.when(jnp.logical_not(later(w)))
        def _(w=w):
            pl.semaphore_signal(
                ready.at[BACK[w]], inc=1, device_id=toward(*WAYS[w]), device_id_type=MESH
            )

    @pl.when(z > 0)
    def _():
        pl.semaphore_signal(ready.at[6], inc=1, device_id=toward("z", -1), device_id_type=MESH)

    def wait_ready(w):
        @pl.when(later(w))
        def _():
            pl.semaphore_wait(ready.at[w], 1)

    def to_partner(i, src, dst):
        return pltpu.make_async_remote_copy(
            src_ref=src, dst_ref=dst, send_sem=part_send.at[i], recv_sem=part_recv.at[i],
            device_id=partner, device_id_type=MESH,
        )

    swaps = [
        to_partner(0, wg_in.at[:, half_other], wg.at[mine]),
        to_partner(1, lg_in, lg.at[mine]),
        to_partner(2, wu_in.at[:, half_other], wu.at[mine]),
        to_partner(3, lu_in, lu.at[mine]),
        to_partner(4, norm, part),
    ]
    for s in swaps[:4]:
        s.start()

    reads[9].wait()
    reads[10].wait()
    lane = lax.broadcasted_iota(jnp.int32, (1, 128), 1)
    first = k * 64 + z * 16
    own = jnp.zeros((1, 128), jnp.float32)
    for i in range(16):
        own = jnp.where(lane == first + i, train[i] + step[i], own)
    norm[chip] = own

    for i in range(3):
        reads[i].wait()
    mix = lax.dot_general(hd[...], ld[...], (((0,), (0,)), ((), ())), preferred_element_type=jnp.float32)
    down[chip, k] = (wd[...].astype(jnp.float32) + mix_rate * mix).astype(jnp.bfloat16)

    def piece(arr, t, c):
        if arr == DOWN:
            return down.at[c, k, pl.ds(16 * t, 16), :]
        ref = gate if arr == GATE else up
        return ref.at[k, t, :, pl.ds(pl.multiple_of(c * 128, 128), 128)]

    def origin(t, a, b):
        dx, dy = (a, b) if TREES[t][0] == "x" else (b, a)
        return lax.rem(y - dy + 4, 4) * 4 + lax.rem(x - dx + 4, 4)

    def way_to(t, a, b, na, nb):
        first_axis, sign = TREES[t]
        second_axis = "y" if first_axis == "x" else "x"
        if na != a:
            return first_axis, (-sign if na == -sign else sign)
        return second_axis, (-sign if nb == -sign else sign)

    def copy_on(arr, t, c, na, nb, to):
        ref = piece(arr, t, c)
        return pltpu.make_async_remote_copy(
            src_ref=ref, dst_ref=ref, send_sem=send_sem.at[arr],
            recv_sem=recv_sem.at[(arr * 4 + t) * 16 + slot_number(na, nb)],
            device_id=to, device_id_type=MESH,
        )

    def send_on(arr, t, a, b, c, only=None):
        for na, nb in onward(a, b, TREES[t][1]):
            way = way_to(t, a, b, na, nb)
            if only is None or way == only:
                copy_on(arr, t, c, na, nb, toward(*way)).start()

    def send_side(arr, t, c):
        ref = piece(arr, t, c)
        pltpu.make_async_remote_copy(
            src_ref=ref, dst_ref=ref, send_sem=side_send.at[arr], recv_sem=side_recv.at[arr],
            device_id=partner, device_id_type=MESH,
        ).start()

    def arrive(arr, t, a, b):
        c = origin(t, a, b)
        copy_on(arr, t, c, a, b, partner).wait_recv()
        send_on(arr, t, a, b, c)
        send_side(arr, t, c)

    def row_copy(rows, w):
        return pltpu.make_async_remote_copy(
            src_ref=norm.at[rows], dst_ref=norm.at[rows], send_sem=n_send.at[w], recv_sem=n_recv.at[w],
            device_id=toward(*WAYS[w]), device_id_type=MESH,
        )

    def row_from(w):
        axis, by = WAYS[w]
        if axis == "x":
            return pl.ds(y * 4 + lax.rem(x - by + 4, 4), 1)
        return pl.ds(lax.rem(y - by + 4, 4) * 4, 4)

    def first_sends(w):
        if w < 2:
            row_copy(pl.ds(chip, 1), w).start()
        for t in range(4):
            send_on(DOWN, t, 0, 0, chip, only=WAYS[w])

    for w in range(4):
        @pl.when(jnp.logical_not(later(w)))
        def _(w=w):
            first_sends(w)

    for w in range(4):
        @pl.when(later(w))
        def _(w=w):
            pl.semaphore_wait(ready.at[w], 1)
            first_sends(w)

    wait_ready(4)
    row_copy(pl.ds(chip, 1), 4).start()
    for t in range(4):
        send_side(DOWN, t, chip)

    def turned(ref, w, low, high):
        for t in range(4):
            cols = pl.ds(256 * t, 256)
            mix = jnp.dot(low[...], high[:, cols], preferred_element_type=jnp.float32)
            full = w[:, cols].astype(jnp.float32) + mix_rate * mix
            ref[k, t, :, pl.ds(pl.multiple_of(chip * 128, 128), 128)] = full.T.astype(jnp.bfloat16)

    for arr, ref, at, args in ((GATE, gate, 0, (wg, lg, hg)), (UP, up, 2, (wu, lu, hu))):
        for i in range(3):
            reads[3 + arr * 3 - 3 + i].wait()
        swaps[at].wait()
        swaps[at + 1].wait()
        turned(ref, *args)
        for t in range(4):
            send_on(arr, t, 0, 0, chip)
            send_side(arr, t, chip)

    def rows_along_y():
        for w in (0, 1, 4):
            row_copy(row_from(w), w).wait_recv()
        wait_ready(5)
        for w in (2, 3, 5):
            row_copy(pl.ds(y * 4, 4), w).start()

    def rows_to_partner():
        for w in (2, 3, 5):
            row_copy(row_from(w), w).wait_recv()
        swaps[4].start()

    def rows_of_chip():
        swaps[4].wait()
        total[...] = norm[...] + part[...]

    def z_copy(src, dst, i, by):
        return pltpu.make_async_remote_copy(
            src_ref=src, dst_ref=dst, send_sem=n_send.at[i], recv_sem=n_recv.at[i],
            device_id=toward("z", by), device_id_type=MESH,
        )

    def z_ends():
        @pl.when(z < 3)
        def _():
            pl.semaphore_wait(ready.at[6], 1)

        @pl.when(z == 0)
        def _():
            z_copy(total, below, 6, 1).start()

        @pl.when(z == 3)
        def _():
            z_copy(total, above, 7, -1).start()

    def z_up_sum():
        @pl.when(z > 0)
        def _():
            z_copy(total, below, 6, 1).wait_recv()
        tosend[0] = total[...] + below[...]

    def z_up_send():
        @pl.when((z > 0) & (z < 3))
        def _():
            z_copy(tosend.at[0], below, 6, 1).start()

    def z_down_sum():
        @pl.when(z < 3)
        def _():
            z_copy(total, above, 7, -1).wait_recv()
        tosend[1] = total[...] + above[...]

    def z_down_send():
        @pl.when((z > 0) & (z < 3))
        def _():
            z_copy(tosend.at[1], above, 7, -1).start()

    def norm_end():
        for w in range(6):
            rows = pl.ds(0, 1) if WAYS[w][0] == "x" else pl.ds(0, 4)
            row_copy(rows, w).wait_send()

        @pl.when(z < 3)
        def _():
            z_copy(total, below, 6, 1).wait_send()

        @pl.when(z > 0)
        def _():
            z_copy(total, above, 7, -1).wait_send()

        norm_out[...] = tosend[0] + above[...]

    def level(hops):
        places = [(a, b) for a, b in tree_slots(1) if abs(a) + abs(b) == hops]
        return [
            (arr, t, TREES[t][1] * a, TREES[t][1] * b)
            for arr in (DOWN, GATE, UP) for a, b in places for t in range(4)
        ]

    events = [e for hops in (1, 2, 3, 4) for e in level(hops)]
    extra = {
        0: rows_along_y, 48: rows_to_partner, 60: rows_of_chip, 72: z_ends,
        96: z_up_sum, 108: z_up_send, 120: z_down_sum, 132: z_down_send, 150: norm_end,
    }
    for n, e in enumerate(events):
        if n in extra:
            extra[n]()
        arrive(*e)

    def drain(arr, sent, other_half, own_half):
        pltpu.make_async_copy(sent, sent, send_sem.at[arr]).wait()
        pltpu.make_async_copy(own_half, own_half, side_send.at[arr]).wait()
        pltpu.make_async_copy(other_half, other_half, side_recv.at[arr]).wait()

    drain(DOWN, down.at[pl.ds(0, 15), k], down.at[:, other], down.at[:, k])
    drain(GATE, gate.at[k, :, :, pl.ds(0, 1920)], gate.at[other], gate.at[k])
    drain(UP, up.at[k, :, :, pl.ds(0, 1920)], up.at[other], up.at[k])


def write_kernel(down, gate, up, norm, down_out, gate_out, up_out, norm_out, sem):
    copies = []
    for n, (src, dst) in enumerate([(gate, gate_out), (up, up_out)]):
        for h in range(2):
            for t in range(4):
                copies.append((src.at[h, t], dst.at[h, t]))
    for q in range(8):
        rows = pl.ds(2 * q, 2)
        copies.append((down.at[rows], down_out.at[rows]))
    copies = [pltpu.make_async_copy(s, d, sem.at[i]) for i, (s, d) in enumerate(copies)]
    for c in copies:
        c.start()
    norm_out[...] = norm[...].reshape(16, 128).astype(jnp.bfloat16)
    for c in copies:
        c.wait()


def local(
    weight_gate, low_gate, high_gate, weight_up, low_up, high_up,
    weight_down, low_down, high_down, norm_train, norm_step,
):
    bf16, f32 = jnp.bfloat16, jnp.float32
    hbm = pl.BlockSpec(memory_space=pltpu.HBM)
    vmem = pl.BlockSpec(memory_space=pltpu.VMEM)
    dma = pltpu.SemaphoreType.DMA
    rows = pltpu.VMEM((16, 1, 128), f32)
    down, gate, up, norm = pl.pallas_call(
        gather_kernel,
        out_shape=(
            pltpu.VMEM((16, 2, 64, 2048), bf16),
            pltpu.VMEM((2, 4, 256, 2048), bf16),
            pltpu.VMEM((2, 4, 256, 2048), bf16),
            pltpu.VMEM((16, 1, 128), f32),
        ),
        in_specs=[hbm] * 11,
        out_specs=(vmem,) * 4,
        scratch_shapes=[
            pltpu.VMEM((64, 2048), bf16), pltpu.VMEM((64, 2048), bf16), pltpu.VMEM((64, 64), bf16),
            pltpu.VMEM((128, 1024), bf16), pltpu.VMEM((128, 64), bf16), pltpu.VMEM((64, 1024), bf16),
            pltpu.VMEM((128, 1024), bf16), pltpu.VMEM((128, 64), bf16), pltpu.VMEM((64, 1024), bf16),
            pltpu.SMEM((16,), f32), pltpu.SMEM((16,), f32),
            rows, rows, rows, rows, rows, pltpu.VMEM((2, 16, 1, 128), f32),
            dma((11,)), dma((5,)), dma((5,)), dma((3,)), dma((3,)), dma((3,)), dma((192,)),
            dma((8,)), dma((8,)), pltpu.SemaphoreType.REGULAR((7,)),
        ],
        compiler_params=pltpu.CompilerParams(
            collective_id=0, has_side_effects=True, vmem_limit_bytes=8 << 20
        ),
        name="gather",
    )(*(
        pltpu.with_memory_space_constraint(a, pltpu.HBM)
        for a in (
            weight_down.T, low_down.T, high_down, weight_gate, low_gate, high_gate,
            weight_up, low_up, high_up, norm_train, norm_step,
        )
    ))
    down, gate, up, norm = pl.pallas_call(
        write_kernel,
        out_shape=(
            jax.ShapeDtypeStruct((16, 2, 64, 2048), bf16),
            jax.ShapeDtypeStruct((2, 4, 256, 2048), bf16),
            jax.ShapeDtypeStruct((2, 4, 256, 2048), bf16),
            jax.ShapeDtypeStruct((16, 128), bf16),
        ),
        in_specs=[vmem] * 4,
        out_specs=(hbm, hbm, hbm, vmem),
        scratch_shapes=[dma((24,))],
        compiler_params=pltpu.CompilerParams(vmem_limit_bytes=4 << 20),
        name="write",
    )(down, gate, up, norm)
    return gate.reshape(2048, 2048), up.reshape(2048, 2048), down.reshape(2048, 2048), norm.reshape(2048)


def solution(mesh):
    split = Mesh(
        mesh.devices.reshape(4, 4, 2, mesh.shape["model"]), ROWS_MODEL
    )
    placed = (
        P(ROWS, "model"),
        P(ROWS, None),
        P(None, "model"),
        P(ROWS, "model"),
        P(ROWS, None),
        P(None, "model"),
        P("model", ROWS),
        P("model", None),
        P(None, ROWS),
        P(ROWS_MODEL),
        P(ROWS_MODEL),
    )
    return jax.shard_map(
        local,
        mesh=split,
        in_specs=placed,
        out_specs=(P("model", None), P("model", None), P(None, "model"), P()),
        check_vma=False,
    )
```

```python
import functools

import jax
import jax.numpy as jnp
from jax import lax
from jax.experimental import pallas as pl
from jax.experimental.pallas import tpu as pltpu
from jax.sharding import Mesh
from jax.sharding import PartitionSpec as P

ROWS = ("rows_0", "rows_1", "rows_2")
ROWS_MODEL = ("rows_0", "rows_1", "rows_2", "model")
MESH = pl.DeviceIdType.MESH

mix_rate = 0.5

TREES = (("x", 1), ("x", -1), ("y", 1), ("y", -1))
DOWN, GATE, UP = 0, 1, 2


def tree_slots(sign):
    steps = (0, sign, -sign, 2 * sign)
    hops = {0: 0, sign: 1, -sign: 1, 2 * sign: 2}
    slots = [(a, b) for a in steps for b in steps if (a, b) != (0, 0)]
    return sorted(slots, key=lambda s: (hops[s[0]] + hops[s[1]], hops[s[1]]))


def onward(a, b, sign):
    places = []
    if b == 0:
        if a == 0:
            places += [(sign, 0), (-sign, 0)]
        elif a == sign:
            places += [(2 * sign, 0)]
        places += [(a, sign), (a, -sign)]
    elif b == sign:
        places += [(a, 2 * sign)]
    return places


def slot_number(a, b):
    return (a % 4) * 4 + b % 4


WAYS = (("x", 1), ("x", -1), ("y", 1), ("y", -1), ("x", 2), ("y", 2))
BACK = (1, 0, 3, 2, 4, 5)


def gather_kernel(
    wd_in, ld_in, hd_in, wg_in, lg_in, hg_in, wu_in, lu_in, hu_in, train_in, step_in,
    down, gate, up, norm_out,
    wd, ld, hd, wg, lg, hg, wu, lu, hu, train, step, norm, part, total, below, above, tosend,
    in_sem, part_send, part_recv, send_sem, side_send, side_recv, recv_sem,
    n_send, n_recv, ready,
):
    y, x, k, z = (lax.axis_index(n) for n in ROWS_MODEL)
    other = 1 - k
    chip = y * 4 + x
    place = {"x": x, "y": y}

    def toward(axis, by):
        if axis == "x":
            return {"rows_1": lax.rem(x + by + 4, 4)}
        if axis == "y":
            return {"rows_0": lax.rem(y + by + 4, 4)}
        return {"model": lax.rem(z + by + 4, 4)}

    partner = {"rows_2": other}

    half = pl.ds(pl.multiple_of(k * 1024, 1024), 1024)
    half_other = pl.ds(pl.multiple_of(other * 1024, 1024), 1024)
    mine = pl.ds(pl.multiple_of(k * 64, 64), 64)
    reads = [
        pltpu.make_async_copy(s, d, in_sem.at[i])
        for i, (s, d) in enumerate(
            [
                (wd_in, wd), (ld_in, ld), (hd_in, hd),
                (wg_in.at[:, half], wg.at[mine]), (lg_in, lg.at[mine]), (hg_in.at[:, half], hg),
                (wu_in.at[:, half], wu.at[mine]), (lu_in, lu.at[mine]), (hu_in.at[:, half], hu),
                (train_in, train), (step_in, step),
            ]
        )
    ]
    for r in reads:
        r.start()
    below[...] = jnp.zeros_like(below)
    above[...] = jnp.zeros_like(above)

    def later(way):
        axis, by = WAYS[way]
        p = place[axis]
        return (p == 0) | (p == 3) if by == -1 else p < 2

    barrier = pltpu.get_barrier_semaphore()
    pl.semaphore_signal(barrier, inc=1, device_id=partner, device_id_type=MESH)
    for w in range(6):
        @pl.when(later(w))
        def _(w=w):
            pl.semaphore_signal(barrier, inc=1, device_id=toward(*WAYS[w]), device_id_type=MESH)

    @pl.when(z < 3)
    def _():
        pl.semaphore_signal(barrier, inc=1, device_id=toward("z", 1), device_id_type=MESH)

    one, nil = jnp.int32(1), jnp.int32(0)
    greetings = 1 + jnp.where(z > 0, one, nil)
    for w in range(6):
        greetings = greetings + jnp.where(later(w), nil, one)
    pl.semaphore_wait(barrier, greetings)
    for w in range(6):
        @pl.when(jnp.logical_not(later(w)))
        def _(w=w):
            pl.semaphore_signal(
                ready.at[BACK[w]], inc=1, device_id=toward(*WAYS[w]), device_id_type=MESH
            )

    @pl.when(z > 0)
    def _():
        pl.semaphore_signal(ready.at[6], inc=1, device_id=toward("z", -1), device_id_type=MESH)

    def wait_ready(w):
        @pl.when(later(w))
        def _():
            pl.semaphore_wait(ready.at[w], 1)

    def to_partner(i, src, dst):
        return pltpu.make_async_remote_copy(
            src_ref=src, dst_ref=dst, send_sem=part_send.at[i], recv_sem=part_recv.at[i],
            device_id=partner, device_id_type=MESH,
        )

    swaps = [
        to_partner(0, wg_in.at[:, half_other], wg.at[mine]),
        to_partner(1, lg_in, lg.at[mine]),
        to_partner(2, wu_in.at[:, half_other], wu.at[mine]),
        to_partner(3, lu_in, lu.at[mine]),
        to_partner(4, norm, part),
    ]
    for s in swaps[:4]:
        s.start()

    def piece(arr, t, c):
        if arr == DOWN:
            return down.at[c, k, pl.ds(16 * t, 16), :]
        ref = gate if arr == GATE else up
        return ref.at[k, t, :, pl.ds(pl.multiple_of(c * 128, 128), 128)]

    def origin(t, a, b):
        dx, dy = (a, b) if TREES[t][0] == "x" else (b, a)
        return lax.rem(y - dy + 4, 4) * 4 + lax.rem(x - dx + 4, 4)

    def way_to(t, a, b, na, nb):
        first_axis, sign = TREES[t]
        second_axis = "y" if first_axis == "x" else "x"
        if na != a:
            return first_axis, (-sign if na == -sign else sign)
        return second_axis, (-sign if nb == -sign else sign)

    def copy_on(arr, t, c, na, nb, to):
        ref = piece(arr, t, c)
        return pltpu.make_async_remote_copy(
            src_ref=ref, dst_ref=ref, send_sem=send_sem.at[arr],
            recv_sem=recv_sem.at[(arr * 4 + t) * 16 + slot_number(na, nb)],
            device_id=to, device_id_type=MESH,
        )

    def send_on(arr, t, a, b, c, only=None):
        for na, nb in onward(a, b, TREES[t][1]):
            way = way_to(t, a, b, na, nb)
            if only is None or way == only:
                copy_on(arr, t, c, na, nb, toward(*way)).start()

    def send_side(arr, t, c):
        ref = piece(arr, t, c)
        pltpu.make_async_remote_copy(
            src_ref=ref, dst_ref=ref, send_sem=side_send.at[arr], recv_sem=side_recv.at[arr],
            device_id=partner, device_id_type=MESH,
        ).start()

    def arrive(arr, t, a, b):
        c = origin(t, a, b)
        copy_on(arr, t, c, a, b, partner).wait_recv()
        send_on(arr, t, a, b, c)
        send_side(arr, t, c)

    def row_copy(rows, w):
        return pltpu.make_async_remote_copy(
            src_ref=norm.at[rows], dst_ref=norm.at[rows], send_sem=n_send.at[w], recv_sem=n_recv.at[w],
            device_id=toward(*WAYS[w]), device_id_type=MESH,
        )

    def row_from(w):
        axis, by = WAYS[w]
        if axis == "x":
            return pl.ds(y * 4 + lax.rem(x - by + 4, 4), 1)
        return pl.ds(lax.rem(y - by + 4, 4) * 4, 4)

    for i in range(3):
        reads[i].wait()
    for t in range(4):
        quarter = pl.ds(16 * t, 16)
        mix = lax.dot_general(
            hd[:, quarter], ld[...], (((0,), (0,)), ((), ())), preferred_element_type=jnp.float32
        )
        full = wd[quarter, :].astype(jnp.float32) + mix_rate * mix
        down[chip, k, quarter, :] = full.astype(jnp.bfloat16)
        for w in range(4):
            @pl.when(jnp.logical_not(later(w)))
            def _(t=t, w=w):
                send_on(DOWN, t, 0, 0, chip, only=WAYS[w])

    for w in range(4):
        @pl.when(later(w))
        def _(w=w):
            pl.semaphore_wait(ready.at[w], 1)
            for t in range(4):
                send_on(DOWN, t, 0, 0, chip, only=WAYS[w])

    for t in range(4):
        send_side(DOWN, t, chip)

    reads[9].wait()
    reads[10].wait()
    lane = lax.broadcasted_iota(jnp.int32, (1, 128), 1)
    first = k * 64 + z * 16
    own = jnp.zeros((1, 128), jnp.float32)
    for i in range(16):
        own = jnp.where(lane == first + i, train[i] + step[i], own)
    norm[chip] = own

    wait_ready(4)
    for w in (0, 1, 4):
        row_copy(pl.ds(chip, 1), w).start()

    def turned(ref, w, low, high):
        for t in range(4):
            cols = pl.ds(256 * t, 256)
            mix = jnp.dot(low[...], high[:, cols], preferred_element_type=jnp.float32)
            full = w[:, cols].astype(jnp.float32) + mix_rate * mix
            ref[k, t, :, pl.ds(pl.multiple_of(chip * 128, 128), 128)] = full.T.astype(jnp.bfloat16)

    for arr, ref, at, args in ((GATE, gate, 0, (wg, lg, hg)), (UP, up, 2, (wu, lu, hu))):
        for i in range(3):
            reads[3 + arr * 3 - 3 + i].wait()
        swaps[at].wait()
        swaps[at + 1].wait()
        turned(ref, *args)
        for t in range(4):
            send_on(arr, t, 0, 0, chip)
            send_side(arr, t, chip)

    def rows_along_y():
        for w in (0, 1, 4):
            row_copy(row_from(w), w).wait_recv()
        wait_ready(5)
        for w in (2, 3, 5):
            row_copy(pl.ds(y * 4, 4), w).start()

    def rows_to_partner():
        for w in (2, 3, 5):
            row_copy(row_from(w), w).wait_recv()
        swaps[4].start()

    def rows_of_chip():
        swaps[4].wait()
        total[...] = norm[...] + part[...]

    def z_copy(src, dst, i, by):
        return pltpu.make_async_remote_copy(
            src_ref=src, dst_ref=dst, send_sem=n_send.at[i], recv_sem=n_recv.at[i],
            device_id=toward("z", by), device_id_type=MESH,
        )

    def z_ends():
        @pl.when(z < 3)
        def _():
            pl.semaphore_wait(ready.at[6], 1)

        @pl.when(z == 0)
        def _():
            z_copy(total, below, 6, 1).start()

        @pl.when(z == 3)
        def _():
            z_copy(total, above, 7, -1).start()

    def z_up_sum():
        @pl.when(z > 0)
        def _():
            z_copy(total, below, 6, 1).wait_recv()
        tosend[0] = total[...] + below[...]

    def z_up_send():
        @pl.when((z > 0) & (z < 3))
        def _():
            z_copy(tosend.at[0], below, 6, 1).start()

    def z_down_sum():
        @pl.when(z < 3)
        def _():
            z_copy(total, above, 7, -1).wait_recv()
        tosend[1] = total[...] + above[...]

    def z_down_send():
        @pl.when((z > 0) & (z < 3))
        def _():
            z_copy(tosend.at[1], above, 7, -1).start()

    def norm_end():
        for w in range(6):
            rows = pl.ds(0, 1) if WAYS[w][0] == "x" else pl.ds(0, 4)
            row_copy(rows, w).wait_send()

        @pl.when(z < 3)
        def _():
            z_copy(total, below, 6, 1).wait_send()

        @pl.when(z > 0)
        def _():
            z_copy(total, above, 7, -1).wait_send()

        norm_out[...] = tosend[0] + above[...]

    def level(hops):
        places = [(a, b) for a, b in tree_slots(1) if abs(a) + abs(b) == hops]
        return [
            (arr, t, TREES[t][1] * a, TREES[t][1] * b)
            for arr in (DOWN, GATE, UP) for a, b in places for t in range(4)
        ]

    events = [e for hops in (1, 2, 3, 4) for e in level(hops)]
    extra = {
        0: rows_along_y, 48: rows_to_partner, 60: rows_of_chip, 72: z_ends,
        96: z_up_sum, 108: z_up_send, 120: z_down_sum, 132: z_down_send, 150: norm_end,
    }
    for n, e in enumerate(events):
        if n in extra:
            extra[n]()
        arrive(*e)

    def drain(arr, sent, other_half, own_half):
        pltpu.make_async_copy(sent, sent, send_sem.at[arr]).wait()
        pltpu.make_async_copy(own_half, own_half, side_send.at[arr]).wait()
        pltpu.make_async_copy(other_half, other_half, side_recv.at[arr]).wait()

    drain(DOWN, down.at[pl.ds(0, 15), k], down.at[:, other], down.at[:, k])
    drain(GATE, gate.at[k, :, :, pl.ds(0, 1920)], gate.at[other], gate.at[k])
    drain(UP, up.at[k, :, :, pl.ds(0, 1920)], up.at[other], up.at[k])


def write_kernel(down, gate, up, norm, down_out, gate_out, up_out, norm_out, rounded, sem):
    rounded[...] = norm[...].reshape(16, 128).astype(jnp.bfloat16)
    copies = []
    for src, dst in ((gate, gate_out), (up, up_out)):
        for h in range(2):
            for t in range(4):
                copies.append((src.at[h, t], dst.at[h, t]))
    for q in range(8):
        rows = pl.ds(2 * q, 2)
        copies.append((down.at[rows], down_out.at[rows]))
    copies.append((rounded, norm_out))
    copies = [pltpu.make_async_copy(s, d, sem.at[i]) for i, (s, d) in enumerate(copies)]
    for c in copies:
        c.start()
    for c in copies:
        c.wait()


def local(
    weight_gate, low_gate, high_gate, weight_up, low_up, high_up,
    weight_down, low_down, high_down, norm_train, norm_step,
):
    bf16, f32 = jnp.bfloat16, jnp.float32
    hbm = pl.BlockSpec(memory_space=pltpu.HBM)
    vmem = pl.BlockSpec(memory_space=pltpu.VMEM)
    dma = pltpu.SemaphoreType.DMA
    rows = pltpu.VMEM((16, 1, 128), f32)
    down, gate, up, norm = pl.pallas_call(
        gather_kernel,
        out_shape=(
            pltpu.VMEM((16, 2, 64, 2048), bf16),
            pltpu.VMEM((2, 4, 256, 2048), bf16),
            pltpu.VMEM((2, 4, 256, 2048), bf16),
            pltpu.VMEM((16, 1, 128), f32),
        ),
        in_specs=[hbm] * 11,
        out_specs=(vmem,) * 4,
        scratch_shapes=[
            pltpu.VMEM((64, 2048), bf16), pltpu.VMEM((64, 2048), bf16), pltpu.VMEM((64, 64), bf16),
            pltpu.VMEM((128, 1024), bf16), pltpu.VMEM((128, 64), bf16), pltpu.VMEM((64, 1024), bf16),
            pltpu.VMEM((128, 1024), bf16), pltpu.VMEM((128, 64), bf16), pltpu.VMEM((64, 1024), bf16),
            pltpu.SMEM((16,), f32), pltpu.SMEM((16,), f32),
            rows, rows, rows, rows, rows, pltpu.VMEM((2, 16, 1, 128), f32),
            dma((11,)), dma((5,)), dma((5,)), dma((3,)), dma((3,)), dma((3,)), dma((192,)),
            dma((8,)), dma((8,)), pltpu.SemaphoreType.REGULAR((7,)),
        ],
        compiler_params=pltpu.CompilerParams(
            collective_id=0, has_side_effects=True, vmem_limit_bytes=8 << 20
        ),
        name="gather",
    )(*(
        pltpu.with_memory_space_constraint(a, pltpu.HBM)
        for a in (
            weight_down.T, low_down.T, high_down, weight_gate, low_gate, high_gate,
            weight_up, low_up, high_up, norm_train, norm_step,
        )
    ))
    down, gate, up, norm = pl.pallas_call(
        write_kernel,
        out_shape=(
            jax.ShapeDtypeStruct((16, 2, 64, 2048), bf16),
            jax.ShapeDtypeStruct((2, 4, 256, 2048), bf16),
            jax.ShapeDtypeStruct((2, 4, 256, 2048), bf16),
            jax.ShapeDtypeStruct((16, 128), bf16),
        ),
        in_specs=[vmem] * 4,
        out_specs=(hbm,) * 4,
        scratch_shapes=[pltpu.VMEM((16, 128), bf16), dma((25,))],
        compiler_params=pltpu.CompilerParams(vmem_limit_bytes=4 << 20),
        name="write",
    )(down, gate, up, norm)
    return gate.reshape(2048, 2048), up.reshape(2048, 2048), down.reshape(2048, 2048), norm.reshape(2048)


def solution(mesh):
    split = Mesh(
        mesh.devices.reshape(4, 4, 2, mesh.shape["model"]), ROWS_MODEL
    )
    placed = (
        P(ROWS, "model"),
        P(ROWS, None),
        P(None, "model"),
        P(ROWS, "model"),
        P(ROWS, None),
        P(None, "model"),
        P("model", ROWS),
        P("model", None),
        P(None, ROWS),
        P(ROWS_MODEL),
        P(ROWS_MODEL),
    )
    return jax.shard_map(
        local,
        mesh=split,
        in_specs=placed,
        out_specs=(P("model", None), P("model", None), P(None, "model"), P()),
        check_vma=False,
    )
```

```python
import functools

import jax
import jax.numpy as jnp
from jax import lax
from jax.experimental import pallas as pl
from jax.experimental.pallas import tpu as pltpu
from jax.sharding import Mesh
from jax.sharding import PartitionSpec as P

ROWS = ("rows_0", "rows_1", "rows_2")
ROWS_MODEL = ("rows_0", "rows_1", "rows_2", "model")
MESH = pl.DeviceIdType.MESH

mix_rate = 0.5

TREES = (("x", 1), ("x", -1), ("y", 1), ("y", -1))
DOWN, GATE, UP = 0, 1, 2


def tree_slots(sign):
    steps = (0, sign, -sign, 2 * sign)
    hops = {0: 0, sign: 1, -sign: 1, 2 * sign: 2}
    slots = [(a, b) for a in steps for b in steps if (a, b) != (0, 0)]
    return sorted(slots, key=lambda s: (hops[s[0]] + hops[s[1]], hops[s[1]]))


def onward(a, b, sign):
    places = []
    if b == 0:
        if a == 0:
            places += [(sign, 0), (-sign, 0)]
        elif a == sign:
            places += [(2 * sign, 0)]
        places += [(a, sign), (a, -sign)]
    elif b == sign:
        places += [(a, 2 * sign)]
    return places


def slot_number(a, b):
    return (a % 4) * 4 + b % 4


WAYS = (("x", 1), ("x", -1), ("y", 1), ("y", -1), ("x", 2), ("y", 2))
BACK = (1, 0, 3, 2, 4, 5)


def gather_kernel(
    wd_in, ld_in, hd_in, wg_in, lg_in, hg_in, wu_in, lu_in, hu_in, train_in, step_in,
    down, gate, up, norm_out,
    wd, ld, hd, wg, lg, hg, wu, lu, hu, train, step, norm, part, total, below, above, tosend,
    in_sem, part_send, part_recv, send_sem, side_send, side_recv, recv_sem,
    n_send, n_recv, ready,
):
    y, x, k, z = (lax.axis_index(n) for n in ROWS_MODEL)
    other = 1 - k
    chip = y * 4 + x
    place = {"x": x, "y": y}

    def toward(axis, by):
        if axis == "x":
            return {"rows_1": lax.rem(x + by + 4, 4)}
        if axis == "y":
            return {"rows_0": lax.rem(y + by + 4, 4)}
        return {"model": lax.rem(z + by + 4, 4)}

    partner = {"rows_2": other}

    def later(way):
        axis, by = WAYS[way]
        p = place[axis]
        return (p == 0) | (p == 3) if by == -1 else p < 2

    barrier = pltpu.get_barrier_semaphore()
    pl.semaphore_signal(barrier, inc=1, device_id=partner, device_id_type=MESH)
    for w in range(6):
        @pl.when(later(w))
        def _(w=w):
            pl.semaphore_signal(barrier, inc=1, device_id=toward(*WAYS[w]), device_id_type=MESH)

    half = pl.ds(pl.multiple_of(k * 1024, 1024), 1024)
    half_other = pl.ds(pl.multiple_of(other * 1024, 1024), 1024)
    mine = pl.ds(pl.multiple_of(k * 64, 64), 64)
    reads = [
        pltpu.make_async_copy(s, d, in_sem.at[i])
        for i, (s, d) in enumerate(
            [
                (wd_in, wd), (ld_in, ld), (hd_in, hd),
                (wg_in.at[:, half], wg.at[mine]), (lg_in, lg.at[mine]), (hg_in.at[:, half], hg),
                (wu_in.at[:, half], wu.at[mine]), (lu_in, lu.at[mine]), (hu_in.at[:, half], hu),
                (train_in, train), (step_in, step),
            ]
        )
    ]
    for r in reads[:3]:
        r.start()
    below[...] = jnp.zeros_like(below)
    above[...] = jnp.zeros_like(above)

    @pl.when(z < 3)
    def _():
        pl.semaphore_signal(barrier, inc=1, device_id=toward("z", 1), device_id_type=MESH)

    one, nil = jnp.int32(1), jnp.int32(0)
    greetings = 1 + jnp.where(z > 0, one, nil)
    for w in range(6):
        greetings = greetings + jnp.where(later(w), nil, one)
    pl.semaphore_wait(barrier, greetings)
    for w in range(6):
        @pl.when(jnp.logical_not(later(w)))
        def _(w=w):
            pl.semaphore_signal(
                ready.at[BACK[w]], inc=1, device_id=toward(*WAYS[w]), device_id_type=MESH
            )

    for r in reads[3:]:
        r.start()

    @pl.when(z > 0)
    def _():
        pl.semaphore_signal(ready.at[6], inc=1, device_id=toward("z", -1), device_id_type=MESH)

    def wait_ready(w):
        @pl.when(later(w))
        def _():
            pl.semaphore_wait(ready.at[w], 1)

    def to_partner(i, src, dst):
        return pltpu.make_async_remote_copy(
            src_ref=src, dst_ref=dst, send_sem=part_send.at[i], recv_sem=part_recv.at[i],
            device_id=partner, device_id_type=MESH,
        )

    swaps = [
        to_partner(0, wg_in.at[:, half_other], wg.at[mine]),
        to_partner(1, lg_in, lg.at[mine]),
        to_partner(2, wu_in.at[:, half_other], wu.at[mine]),
        to_partner(3, lu_in, lu.at[mine]),
        to_partner(4, norm, part),
    ]
    for s in swaps[:4]:
        s.start()

    def piece(arr, t, c, h):
        if arr == DOWN:
            return down.at[c, h, pl.ds(16 * t, 16), :]
        ref = gate if arr == GATE else up
        return ref.at[h, t, :, pl.ds(pl.multiple_of(c * 128, 128), 128)]

    def origin(t, a, b):
        dx, dy = (a, b) if TREES[t][0] == "x" else (b, a)
        return lax.rem(y - dy + 4, 4) * 4 + lax.rem(x - dx + 4, 4)

    def way_to(t, a, b, na, nb):
        first_axis, sign = TREES[t]
        second_axis = "y" if first_axis == "x" else "x"
        if na != a:
            return first_axis, (-sign if na == -sign else sign)
        return second_axis, (-sign if nb == -sign else sign)

    def copy_on(arr, t, c, na, nb, to, h):
        ref = piece(arr, t, c, h)
        number = slot_number(na, nb)
        if abs(na) + abs(nb) == 4:
            to, number = {**to, "rows_2": 1}, number * h
        return pltpu.make_async_remote_copy(
            src_ref=ref, dst_ref=ref, send_sem=send_sem.at[arr],
            recv_sem=recv_sem.at[(arr * 4 + t) * 16 + number],
            device_id=to, device_id_type=MESH,
        )

    def send_on(arr, t, a, b, c, only=None):
        for na, nb in onward(a, b, TREES[t][1]):
            way = way_to(t, a, b, na, nb)
            if only is None or way == only:
                copy_on(arr, t, c, na, nb, toward(*way), k).start()

    def send_side(arr, t, c, h=None):
        ref = piece(arr, t, c, k if h is None else h)
        sem = arr if h is None else 3 + arr
        pltpu.make_async_remote_copy(
            src_ref=ref, dst_ref=ref, send_sem=side_send.at[sem], recv_sem=side_recv.at[sem],
            device_id=partner, device_id_type=MESH,
        ).start()

    def arrive(arr, t, a, b):
        c = origin(t, a, b)
        copy_on(arr, t, c, a, b, partner, k).wait_recv()
        send_on(arr, t, a, b, c)
        send_side(arr, t, c)

    def arrive_last(arr, t, a, b):
        c = origin(t, a, b)
        copy_on(arr, t, c, a, b, {}, 1).wait_recv()
        send_side(arr, t, c)
        copy_on(arr, t, c, a, b, {}, 0).wait_recv()
        send_side(arr, t, c, 0)

    def row_copy(rows, w):
        return pltpu.make_async_remote_copy(
            src_ref=norm.at[rows], dst_ref=norm.at[rows], send_sem=n_send.at[w], recv_sem=n_recv.at[w],
            device_id=toward(*WAYS[w]), device_id_type=MESH,
        )

    def row_from(w):
        axis, by = WAYS[w]
        if axis == "x":
            return pl.ds(y * 4 + lax.rem(x - by + 4, 4), 1)
        return pl.ds(lax.rem(y - by + 4, 4) * 4, 4)

    for i in range(3):
        reads[i].wait()
    for t in range(4):
        quarter = pl.ds(16 * t, 16)
        mix = lax.dot_general(
            hd[:, quarter], ld[...], (((0,), (0,)), ((), ())), preferred_element_type=jnp.float32
        )
        full = wd[quarter, :].astype(jnp.float32) + mix_rate * mix
        down[chip, k, quarter, :] = full.astype(jnp.bfloat16)
        for w in range(4):
            @pl.when(jnp.logical_not(later(w)))
            def _(t=t, w=w):
                send_on(DOWN, t, 0, 0, chip, only=WAYS[w])

    for w in range(4):
        @pl.when(later(w))
        def _(w=w):
            pl.semaphore_wait(ready.at[w], 1)
            for t in range(4):
                send_on(DOWN, t, 0, 0, chip, only=WAYS[w])

    for t in range(4):
        send_side(DOWN, t, chip)

    reads[9].wait()
    reads[10].wait()
    lane = lax.broadcasted_iota(jnp.int32, (1, 128), 1)
    first = k * 64 + z * 16
    own = jnp.zeros((1, 128), jnp.float32)
    for i in range(16):
        own = jnp.where(lane == first + i, train[i] + step[i], own)
    norm[chip] = own

    wait_ready(4)
    for w in (0, 1, 4):
        row_copy(pl.ds(chip, 1), w).start()

    def turned(ref, w, low, high):
        for t in range(4):
            cols = pl.ds(256 * t, 256)
            mix = jnp.dot(low[...], high[:, cols], preferred_element_type=jnp.float32)
            full = w[:, cols].astype(jnp.float32) + mix_rate * mix
            ref[k, t, :, pl.ds(pl.multiple_of(chip * 128, 128), 128)] = full.T.astype(jnp.bfloat16)

    for arr, ref, at, args in ((GATE, gate, 0, (wg, lg, hg)), (UP, up, 2, (wu, lu, hu))):
        for i in range(3):
            reads[3 + arr * 3 - 3 + i].wait()
        swaps[at].wait()
        swaps[at + 1].wait()
        turned(ref, *args)
        for t in range(4):
            send_on(arr, t, 0, 0, chip)
            send_side(arr, t, chip)

    def rows_along_y():
        for w in (0, 1, 4):
            row_copy(row_from(w), w).wait_recv()
        wait_ready(5)
        for w in (2, 3, 5):
            row_copy(pl.ds(y * 4, 4), w).start()

    def rows_to_partner():
        for w in (2, 3, 5):
            row_copy(row_from(w), w).wait_recv()
        swaps[4].start()

    def rows_of_chip():
        swaps[4].wait()
        total[...] = norm[...] + part[...]

    def z_copy(src, dst, i, by):
        return pltpu.make_async_remote_copy(
            src_ref=src, dst_ref=dst, send_sem=n_send.at[i], recv_sem=n_recv.at[i],
            device_id=toward("z", by), device_id_type=MESH,
        )

    def z_ends():
        @pl.when(z < 3)
        def _():
            pl.semaphore_wait(ready.at[6], 1)

        @pl.when(z == 0)
        def _():
            z_copy(total, below, 6, 1).start()

        @pl.when(z == 3)
        def _():
            z_copy(total, above, 7, -1).start()

    def z_up_sum():
        @pl.when(z > 0)
        def _():
            z_copy(total, below, 6, 1).wait_recv()
        tosend[0] = total[...] + below[...]

    def z_up_send():
        @pl.when((z > 0) & (z < 3))
        def _():
            z_copy(tosend.at[0], below, 6, 1).start()

    def z_down_sum():
        @pl.when(z < 3)
        def _():
            z_copy(total, above, 7, -1).wait_recv()
        tosend[1] = total[...] + above[...]

    def z_down_send():
        @pl.when((z > 0) & (z < 3))
        def _():
            z_copy(tosend.at[1], above, 7, -1).start()

    def norm_end():
        for w in range(6):
            rows = pl.ds(0, 1) if WAYS[w][0] == "x" else pl.ds(0, 4)
            row_copy(rows, w).wait_send()

        @pl.when(z < 3)
        def _():
            z_copy(total, below, 6, 1).wait_send()

        @pl.when(z > 0)
        def _():
            z_copy(total, above, 7, -1).wait_send()

        norm_out[...] = tosend[0] + above[...]

    def level(hops):
        places = [(a, b) for a, b in tree_slots(1) if abs(a) + abs(b) == hops]
        return [
            (arr, t, TREES[t][1] * a, TREES[t][1] * b)
            for arr in (DOWN, GATE, UP) for a, b in places for t in range(4)
        ]

    events = [e for hops in (1, 2, 3) for e in level(hops)]
    extra = {
        0: rows_along_y, 48: rows_to_partner, 60: rows_of_chip, 72: z_ends,
        96: z_up_sum, 108: z_up_send, 120: z_down_sum, 132: z_down_send, 150: norm_end,
    }
    for n, e in enumerate(events):
        if n in extra:
            extra[n]()
        arrive(*e)

    @pl.when(k == 1)
    def _():
        for e in level(4):
            arrive_last(*e)

    def wait_for(ref, sem):
        pltpu.make_async_copy(ref, ref, sem).wait()

    def most(arr, h):
        if arr == DOWN:
            return down.at[pl.ds(0, 15), h]
        return (gate if arr == GATE else up).at[h, :, :, pl.ds(0, 1920)]

    def whole(arr, h):
        return down.at[:, h] if arr == DOWN else (gate if arr == GATE else up).at[h]

    last = down.at[0, 0]
    for arr in (DOWN, GATE, UP):
        wait_for(most(arr, k), send_sem.at[arr])

    @pl.when(k == 1)
    def _():
        for arr in (DOWN, GATE, UP):
            wait_for(most(arr, 0), side_recv.at[arr])
            wait_for(whole(arr, 1), side_send.at[arr])
            wait_for(last, side_send.at[3 + arr])

    @pl.when(k == 0)
    def _():
        for arr in (DOWN, GATE, UP):
            wait_for(most(arr, 0), side_send.at[arr])
            wait_for(whole(arr, 1), side_recv.at[arr])
            wait_for(last, side_recv.at[3 + arr])


def write_kernel(down, gate, up, norm, down_out, gate_out, up_out, norm_out, rounded, sem):
    copies = []
    for src, dst in ((gate, gate_out), (up, up_out)):
        for h in range(2):
            for t in range(4):
                copies.append((src.at[h, t], dst.at[h, t]))
    for q in range(8):
        rows = pl.ds(2 * q, 2)
        copies.append((down.at[rows], down_out.at[rows]))
    copies.append((rounded, norm_out))
    copies = [pltpu.make_async_copy(s, d, sem.at[i]) for i, (s, d) in enumerate(copies)]
    for c in copies[:-1]:
        c.start()
    rounded[...] = norm[...].reshape(16, 128).astype(jnp.bfloat16)
    copies[-1].start()
    for c in copies:
        c.wait()


def local(
    weight_gate, low_gate, high_gate, weight_up, low_up, high_up,
    weight_down, low_down, high_down, norm_train, norm_step,
):
    bf16, f32 = jnp.bfloat16, jnp.float32
    hbm = pl.BlockSpec(memory_space=pltpu.HBM)
    vmem = pl.BlockSpec(memory_space=pltpu.VMEM)
    dma = pltpu.SemaphoreType.DMA
    rows = pltpu.VMEM((16, 1, 128), f32)
    down, gate, up, norm = pl.pallas_call(
        gather_kernel,
        out_shape=(
            pltpu.VMEM((16, 2, 64, 2048), bf16),
            pltpu.VMEM((2, 4, 256, 2048), bf16),
            pltpu.VMEM((2, 4, 256, 2048), bf16),
            pltpu.VMEM((16, 1, 128), f32),
        ),
        in_specs=[hbm] * 11,
        out_specs=(vmem,) * 4,
        scratch_shapes=[
            pltpu.VMEM((64, 2048), bf16), pltpu.VMEM((64, 2048), bf16), pltpu.VMEM((64, 64), bf16),
            pltpu.VMEM((128, 1024), bf16), pltpu.VMEM((128, 64), bf16), pltpu.VMEM((64, 1024), bf16),
            pltpu.VMEM((128, 1024), bf16), pltpu.VMEM((128, 64), bf16), pltpu.VMEM((64, 1024), bf16),
            pltpu.SMEM((16,), f32), pltpu.SMEM((16,), f32),
            rows, rows, rows, rows, rows, pltpu.VMEM((2, 16, 1, 128), f32),
            dma((11,)), dma((5,)), dma((5,)), dma((3,)), dma((6,)), dma((6,)), dma((192,)),
            dma((8,)), dma((8,)), pltpu.SemaphoreType.REGULAR((7,)),
        ],
        compiler_params=pltpu.CompilerParams(
            collective_id=0, has_side_effects=True, vmem_limit_bytes=8 << 20
        ),
        name="gather",
    )(*(
        pltpu.with_memory_space_constraint(a, pltpu.HBM)
        for a in (
            weight_down.T, low_down.T, high_down, weight_gate, low_gate, high_gate,
            weight_up, low_up, high_up, norm_train, norm_step,
        )
    ))
    down, gate, up, norm = pl.pallas_call(
        write_kernel,
        out_shape=(
            jax.ShapeDtypeStruct((16, 2, 64, 2048), bf16),
            jax.ShapeDtypeStruct((2, 4, 256, 2048), bf16),
            jax.ShapeDtypeStruct((2, 4, 256, 2048), bf16),
            jax.ShapeDtypeStruct((16, 128), bf16),
        ),
        in_specs=[vmem] * 4,
        out_specs=(hbm,) * 4,
        scratch_shapes=[pltpu.VMEM((16, 128), bf16), dma((25,))],
        compiler_params=pltpu.CompilerParams(vmem_limit_bytes=4 << 20),
        name="write",
    )(down, gate, up, norm)
    return gate.reshape(2048, 2048), up.reshape(2048, 2048), down.reshape(2048, 2048), norm.reshape(2048)


def solution(mesh):
    split = Mesh(
        mesh.devices.reshape(4, 4, 2, mesh.shape["model"]), ROWS_MODEL
    )
    placed = (
        P(ROWS, "model"),
        P(ROWS, None),
        P(None, "model"),
        P(ROWS, "model"),
        P(ROWS, None),
        P(None, "model"),
        P("model", ROWS),
        P("model", None),
        P(None, ROWS),
        P(ROWS_MODEL),
        P(ROWS_MODEL),
    )
    return jax.shard_map(
        local,
        mesh=split,
        in_specs=placed,
        out_specs=(P("model", None), P("model", None), P(None, "model"), P()),
        check_vma=False,
    )
```

```python
import functools

import jax
import jax.numpy as jnp
from jax import lax
from jax.experimental import pallas as pl
from jax.experimental.pallas import tpu as pltpu
from jax.sharding import Mesh
from jax.sharding import PartitionSpec as P

ROWS = ("rows_0", "rows_1", "rows_2")
ROWS_MODEL = ("rows_0", "rows_1", "rows_2", "model")
MESH = pl.DeviceIdType.MESH

mix_rate = 0.5

TREES = (("x", 1), ("x", -1), ("y", 1), ("y", -1))
DOWN, GATE, UP = 0, 1, 2


def tree_slots(sign):
    steps = (0, sign, -sign, 2 * sign)
    hops = {0: 0, sign: 1, -sign: 1, 2 * sign: 2}
    slots = [(a, b) for a in steps for b in steps if (a, b) != (0, 0)]
    return sorted(slots, key=lambda s: (hops[s[0]] + hops[s[1]], hops[s[1]]))


def onward(a, b, sign):
    places = []
    if b == 0:
        if a == 0:
            places += [(sign, 0), (-sign, 0)]
        elif a == sign:
            places += [(2 * sign, 0)]
        places += [(a, sign), (a, -sign)]
    elif b == sign:
        places += [(a, 2 * sign)]
    return places


def slot_number(a, b):
    return (a % 4) * 4 + b % 4


WAYS = (("x", 1), ("x", -1), ("y", 1), ("y", -1), ("x", 2), ("y", 2))
BACK = (1, 0, 3, 2, 4, 5)


def gather_kernel(
    wd_in, ld_in, hd_in, wg_in, lg_in, hg_in, wu_in, lu_in, hu_in, train_in, step_in,
    down, gate, up, norm_out,
    wd, ld, hd, wg, lg, hg, wu, lu, hu, train, step, norm, part, total, below, above, tosend,
    in_sem, part_send, part_recv, send_sem, side_send, side_recv, recv_sem,
    n_send, n_recv, ready,
):
    y, x, k, z = (lax.axis_index(n) for n in ROWS_MODEL)
    other = 1 - k
    chip = y * 4 + x
    place = {"x": x, "y": y}

    def toward(axis, by):
        if axis == "x":
            return {"rows_1": lax.rem(x + by + 4, 4)}
        if axis == "y":
            return {"rows_0": lax.rem(y + by + 4, 4)}
        return {"model": lax.rem(z + by + 4, 4)}

    partner = {"rows_2": other}

    def later(way):
        axis, by = WAYS[way]
        p = place[axis]
        return (p == 0) | (p == 3) if by == -1 else p < 2

    barrier = pltpu.get_barrier_semaphore()
    pl.semaphore_signal(barrier, inc=1, device_id=partner, device_id_type=MESH)
    for w in range(6):
        @pl.when(later(w))
        def _(w=w):
            pl.semaphore_signal(barrier, inc=1, device_id=toward(*WAYS[w]), device_id_type=MESH)

    half = pl.ds(pl.multiple_of(k * 1024, 1024), 1024)
    half_other = pl.ds(pl.multiple_of(other * 1024, 1024), 1024)
    mine = pl.ds(pl.multiple_of(k * 64, 64), 64)
    reads = [
        pltpu.make_async_copy(s, d, in_sem.at[i])
        for i, (s, d) in enumerate(
            [
                (wd_in, wd), (ld_in, ld), (hd_in, hd),
                (wg_in.at[:, half], wg.at[mine]), (lg_in, lg.at[mine]), (hg_in.at[:, half], hg),
                (wu_in.at[:, half], wu.at[mine]), (lu_in, lu.at[mine]), (hu_in.at[:, half], hu),
                (train_in, train), (step_in, step),
            ]
        )
    ]
    for r in reads[:3]:
        r.start()
    below[...] = jnp.zeros_like(below)
    above[...] = jnp.zeros_like(above)

    @pl.when(z < 3)
    def _():
        pl.semaphore_signal(barrier, inc=1, device_id=toward("z", 1), device_id_type=MESH)

    one, nil = jnp.int32(1), jnp.int32(0)
    greetings = 1 + jnp.where(z > 0, one, nil)
    for w in range(6):
        greetings = greetings + jnp.where(later(w), nil, one)
    pl.semaphore_wait(barrier, greetings)
    for w in range(6):
        @pl.when(jnp.logical_not(later(w)))
        def _(w=w):
            pl.semaphore_signal(
                ready.at[BACK[w]], inc=1, device_id=toward(*WAYS[w]), device_id_type=MESH
            )

    for r in reads[3:]:
        r.start()

    @pl.when(z > 0)
    def _():
        pl.semaphore_signal(ready.at[6], inc=1, device_id=toward("z", -1), device_id_type=MESH)

    def wait_ready(w):
        @pl.when(later(w))
        def _():
            pl.semaphore_wait(ready.at[w], 1)

    def to_partner(i, src, dst):
        return pltpu.make_async_remote_copy(
            src_ref=src, dst_ref=dst, send_sem=part_send.at[i], recv_sem=part_recv.at[i],
            device_id=partner, device_id_type=MESH,
        )

    swaps = [
        to_partner(0, wg_in.at[:, half_other], wg.at[mine]),
        to_partner(1, lg_in, lg.at[mine]),
        to_partner(2, wu_in.at[:, half_other], wu.at[mine]),
        to_partner(3, lu_in, lu.at[mine]),
        to_partner(4, norm, part),
    ]
    for s in swaps[:4]:
        s.start()

    def piece(arr, t, c):
        if arr == DOWN:
            return down.at[c, k, pl.ds(16 * t, 16), :]
        ref = gate if arr == GATE else up
        return ref.at[k, t, :, pl.ds(pl.multiple_of(c * 128, 128), 128)]

    def origin(t, a, b):
        dx, dy = (a, b) if TREES[t][0] == "x" else (b, a)
        return lax.rem(y - dy + 4, 4) * 4 + lax.rem(x - dx + 4, 4)

    def way_to(t, a, b, na, nb):
        first_axis, sign = TREES[t]
        second_axis = "y" if first_axis == "x" else "x"
        if na != a:
            return first_axis, (-sign if na == -sign else sign)
        return second_axis, (-sign if nb == -sign else sign)

    def copy_on(arr, t, c, na, nb, to):
        ref = piece(arr, t, c)
        return pltpu.make_async_remote_copy(
            src_ref=ref, dst_ref=ref, send_sem=send_sem.at[arr],
            recv_sem=recv_sem.at[(arr * 4 + t) * 16 + slot_number(na, nb)],
            device_id=to, device_id_type=MESH,
        )

    def send_on(arr, t, a, b, c, only=None):
        for na, nb in onward(a, b, TREES[t][1]):
            way = way_to(t, a, b, na, nb)
            if only is None or way == only:
                copy_on(arr, t, c, na, nb, toward(*way)).start()

    def send_side(arr, t, c):
        ref = piece(arr, t, c)
        pltpu.make_async_remote_copy(
            src_ref=ref, dst_ref=ref, send_sem=side_send.at[arr], recv_sem=side_recv.at[arr],
            device_id=partner, device_id_type=MESH,
        ).start()

    def arrive(arr, t, a, b):
        c = origin(t, a, b)
        copy_on(arr, t, c, a, b, partner).wait_recv()
        send_side(arr, t, c)
        send_on(arr, t, a, b, c)

    def row_copy(rows, w):
        return pltpu.make_async_remote_copy(
            src_ref=norm.at[rows], dst_ref=norm.at[rows], send_sem=n_send.at[w], recv_sem=n_recv.at[w],
            device_id=toward(*WAYS[w]), device_id_type=MESH,
        )

    def row_from(w):
        axis, by = WAYS[w]
        if axis == "x":
            return pl.ds(y * 4 + lax.rem(x - by + 4, 4), 1)
        return pl.ds(lax.rem(y - by + 4, 4) * 4, 4)

    for i in range(3):
        reads[i].wait()
    for t in range(4):
        quarter = pl.ds(16 * t, 16)
        mix = lax.dot_general(
            hd[:, quarter], ld[...], (((0,), (0,)), ((), ())), preferred_element_type=jnp.float32
        )
        full = wd[quarter, :].astype(jnp.float32) + mix_rate * mix
        down[chip, k, quarter, :] = full.astype(jnp.bfloat16)
        for w in range(4):
            @pl.when(jnp.logical_not(later(w)))
            def _(t=t, w=w):
                send_on(DOWN, t, 0, 0, chip, only=WAYS[w])

    for w in range(4):
        @pl.when(later(w))
        def _(w=w):
            pl.semaphore_wait(ready.at[w], 1)
            for t in range(4):
                send_on(DOWN, t, 0, 0, chip, only=WAYS[w])

    reads[9].wait()
    reads[10].wait()
    lane = lax.broadcasted_iota(jnp.int32, (1, 128), 1)
    first = k * 64 + z * 16
    own = jnp.zeros((1, 128), jnp.float32)
    for i in range(16):
        own = jnp.where(lane == first + i, train[i] + step[i], own)
    norm[chip] = own

    wait_ready(4)
    for w in (0, 1, 4):
        row_copy(pl.ds(chip, 1), w).start()

    def turned(ref, w, low, high):
        for t in range(4):
            cols = pl.ds(256 * t, 256)
            mix = jnp.dot(low[...], high[:, cols], preferred_element_type=jnp.float32)
            full = w[:, cols].astype(jnp.float32) + mix_rate * mix
            ref[k, t, :, pl.ds(pl.multiple_of(chip * 128, 128), 128)] = full.T.astype(jnp.bfloat16)

    for arr, ref, at, args in ((GATE, gate, 0, (wg, lg, hg)), (UP, up, 2, (wu, lu, hu))):
        for i in range(3):
            reads[3 + arr * 3 - 3 + i].wait()
        swaps[at].wait()
        swaps[at + 1].wait()
        turned(ref, *args)
        for t in range(4):
            send_on(arr, t, 0, 0, chip)

    def rows_along_y():
        for w in (0, 1, 4):
            row_copy(row_from(w), w).wait_recv()
        wait_ready(5)
        for w in (2, 3, 5):
            row_copy(pl.ds(y * 4, 4), w).start()

    def rows_to_partner():
        for arr in (DOWN, GATE, UP):
            for t in range(4):
                send_side(arr, t, chip)
        for w in (2, 3, 5):
            row_copy(row_from(w), w).wait_recv()
        swaps[4].start()

    def rows_of_chip():
        swaps[4].wait()
        total[...] = norm[...] + part[...]

    def z_copy(src, dst, i, by):
        return pltpu.make_async_remote_copy(
            src_ref=src, dst_ref=dst, send_sem=n_send.at[i], recv_sem=n_recv.at[i],
            device_id=toward("z", by), device_id_type=MESH,
        )

    def z_ends():
        @pl.when(z < 3)
        def _():
            pl.semaphore_wait(ready.at[6], 1)

        @pl.when(z == 0)
        def _():
            z_copy(total, below, 6, 1).start()

        @pl.when(z == 3)
        def _():
            z_copy(total, above, 7, -1).start()

    def z_up_sum():
        @pl.when(z > 0)
        def _():
            z_copy(total, below, 6, 1).wait_recv()
        tosend[0] = total[...] + below[...]

    def z_up_send():
        @pl.when((z > 0) & (z < 3))
        def _():
            z_copy(tosend.at[0], below, 6, 1).start()

    def z_down_sum():
        @pl.when(z < 3)
        def _():
            z_copy(total, above, 7, -1).wait_recv()
        tosend[1] = total[...] + above[...]

    def z_down_send():
        @pl.when((z > 0) & (z < 3))
        def _():
            z_copy(tosend.at[1], above, 7, -1).start()

    def norm_end():
        for w in range(6):
            rows = pl.ds(0, 1) if WAYS[w][0] == "x" else pl.ds(0, 4)
            row_copy(rows, w).wait_send()

        @pl.when(z < 3)
        def _():
            z_copy(total, below, 6, 1).wait_send()

        @pl.when(z > 0)
        def _():
            z_copy(total, above, 7, -1).wait_send()

        norm_out[...] = tosend[0] + above[...]

    def level(hops):
        places = [(a, b) for a, b in tree_slots(1) if abs(a) + abs(b) == hops]
        return [
            (arr, t, TREES[t][1] * a, TREES[t][1] * b)
            for arr in (DOWN, GATE, UP) for a, b in places for t in range(4)
        ]

    events = [e for hops in (1, 2, 3, 4) for e in level(hops)]
    extra = {
        0: rows_along_y, 48: rows_to_partner, 60: rows_of_chip, 72: z_ends,
        96: z_up_sum, 108: z_up_send, 120: z_down_sum, 132: z_down_send, 150: norm_end,
    }
    for n, e in enumerate(events):
        if n in extra:
            extra[n]()
        arrive(*e)

    def drain(arr, sent, other_half, own_half):
        pltpu.make_async_copy(sent, sent, send_sem.at[arr]).wait()
        pltpu.make_async_copy(own_half, own_half, side_send.at[arr]).wait()
        pltpu.make_async_copy(other_half, other_half, side_recv.at[arr]).wait()

    drain(DOWN, down.at[pl.ds(0, 15), k], down.at[:, other], down.at[:, k])
    drain(GATE, gate.at[k, :, :, pl.ds(0, 1920)], gate.at[other], gate.at[k])
    drain(UP, up.at[k, :, :, pl.ds(0, 1920)], up.at[other], up.at[k])


def write_kernel(down, gate, up, norm, down_out, gate_out, up_out, norm_out, rounded, sem):
    copies = []
    for src, dst in ((gate, gate_out), (up, up_out)):
        for h in range(2):
            for t in range(4):
                copies.append((src.at[h, t], dst.at[h, t]))
    for q in range(8):
        rows = pl.ds(2 * q, 2)
        copies.append((down.at[rows], down_out.at[rows]))
    copies.append((rounded, norm_out))
    copies = [pltpu.make_async_copy(s, d, sem.at[i]) for i, (s, d) in enumerate(copies)]
    for c in copies[:-1]:
        c.start()
    rounded[...] = norm[...].reshape(16, 128).astype(jnp.bfloat16)
    copies[-1].start()
    for c in copies:
        c.wait()


def local(
    weight_gate, low_gate, high_gate, weight_up, low_up, high_up,
    weight_down, low_down, high_down, norm_train, norm_step,
):
    bf16, f32 = jnp.bfloat16, jnp.float32
    hbm = pl.BlockSpec(memory_space=pltpu.HBM)
    vmem = pl.BlockSpec(memory_space=pltpu.VMEM)
    dma = pltpu.SemaphoreType.DMA
    rows = pltpu.VMEM((16, 1, 128), f32)
    down, gate, up, norm = pl.pallas_call(
        gather_kernel,
        out_shape=(
            pltpu.VMEM((16, 2, 64, 2048), bf16),
            pltpu.VMEM((2, 4, 256, 2048), bf16),
            pltpu.VMEM((2, 4, 256, 2048), bf16),
            pltpu.VMEM((16, 1, 128), f32),
        ),
        in_specs=[hbm] * 11,
        out_specs=(vmem,) * 4,
        scratch_shapes=[
            pltpu.VMEM((64, 2048), bf16), pltpu.VMEM((64, 2048), bf16), pltpu.VMEM((64, 64), bf16),
            pltpu.VMEM((128, 1024), bf16), pltpu.VMEM((128, 64), bf16), pltpu.VMEM((64, 1024), bf16),
            pltpu.VMEM((128, 1024), bf16), pltpu.VMEM((128, 64), bf16), pltpu.VMEM((64, 1024), bf16),
            pltpu.SMEM((16,), f32), pltpu.SMEM((16,), f32),
            rows, rows, rows, rows, rows, pltpu.VMEM((2, 16, 1, 128), f32),
            dma((11,)), dma((5,)), dma((5,)), dma((3,)), dma((3,)), dma((3,)), dma((192,)),
            dma((8,)), dma((8,)), pltpu.SemaphoreType.REGULAR((7,)),
        ],
        compiler_params=pltpu.CompilerParams(
            collective_id=0, has_side_effects=True, vmem_limit_bytes=8 << 20
        ),
        name="gather",
    )(*(
        pltpu.with_memory_space_constraint(a, pltpu.HBM)
        for a in (
            weight_down.T, low_down.T, high_down, weight_gate, low_gate, high_gate,
            weight_up, low_up, high_up, norm_train, norm_step,
        )
    ))
    down, gate, up, norm = pl.pallas_call(
        write_kernel,
        out_shape=(
            jax.ShapeDtypeStruct((16, 2, 64, 2048), bf16),
            jax.ShapeDtypeStruct((2, 4, 256, 2048), bf16),
            jax.ShapeDtypeStruct((2, 4, 256, 2048), bf16),
            jax.ShapeDtypeStruct((16, 128), bf16),
        ),
        in_specs=[vmem] * 4,
        out_specs=(hbm,) * 4,
        scratch_shapes=[pltpu.VMEM((16, 128), bf16), dma((25,))],
        compiler_params=pltpu.CompilerParams(vmem_limit_bytes=4 << 20),
        name="write",
    )(down, gate, up, norm)
    return gate.reshape(2048, 2048), up.reshape(2048, 2048), down.reshape(2048, 2048), norm.reshape(2048)


def solution(mesh):
    split = Mesh(
        mesh.devices.reshape(4, 4, 2, mesh.shape["model"]), ROWS_MODEL
    )
    placed = (
        P(ROWS, "model"),
        P(ROWS, None),
        P(None, "model"),
        P(ROWS, "model"),
        P(ROWS, None),
        P(None, "model"),
        P("model", ROWS),
        P("model", None),
        P(None, ROWS),
        P(ROWS_MODEL),
        P(ROWS_MODEL),
    )
    return jax.shard_map(
        local,
        mesh=split,
        in_specs=placed,
        out_specs=(P("model", None), P("model", None), P(None, "model"), P()),
        check_vma=False,
    )
```
